32 devices in a mesh: dp: 1 (over z), tp: 32 (over y, x, core).
Axes of the slice: x: 4, y: 4, z: 1, core: 2. Of those that a mesh axis runs over, the one named last changes fastest.
The devices are a block of a 4x4x8 slice.
Arguments:
- act_in: bfloat16 [512, 4096], P('dp')
- w_qkv: bfloat16 [3, 4096, 32, 3, 128], P(None, None, 'tp')
- w_out: bfloat16 [3, 32, 128, 4096], P(None, 'tp')
- w_up: bfloat16 [3, 4096, 16384], P(None, None, 'tp')
- w_down: bfloat16 [3, 16384, 4096], P(None, 'tp')
- gain_one: float32 [3, 4096], replicated
- gain_two: float32 [3, 4096], replicated
Outputs:
- output: bfloat16 [512, 4096], P('dp')
All inputs are finite; a program needn't handle non-finite values.
Results may differ from the reference program's by a relative error of at most 0.02.
Values are sent between devices in bfloat16 or wider.
A program may use at most 768 MiB of HBM per device.

```python
import math
import jax
import jax.numpy as jnp
from jax import lax

SEQ_LEN = 512
MODEL_DIM = 4096
NUM_HEADS = 32
FFN_DIM = 16384
NUM_LAYERS = 3

HEAD_DIM = MODEL_DIM // NUM_HEADS
SCORE_SCALE = 1.0 / math.sqrt(HEAD_DIM)
ROW_BLOCK = math.gcd(SEQ_LEN, 2 ** int(math.log2(max(8, 2 ** 24 // (NUM_HEADS * SEQ_LEN)))))


def setup_inputs(seed: int = 0, part: int = 0) -> dict:
    part_key = jax.random.fold_in(jax.random.key(seed), part)
    key_common, key_noise = jax.random.split(part_key)
    shared_mean = jax.random.normal(key_common, (1, MODEL_DIM), jnp.float32)
    token_noise = jax.random.normal(key_noise, (SEQ_LEN, MODEL_DIM), jnp.float32)
    weight_keys = jax.random.split(jax.random.key(seed + 1), 6)
    w_qkv = jax.random.normal(weight_keys[0], (NUM_LAYERS, MODEL_DIM, NUM_HEADS, 3, HEAD_DIM), jnp.float32) * MODEL_DIM ** -0.5
    w_out = jax.random.normal(weight_keys[1], (NUM_LAYERS, NUM_HEADS, HEAD_DIM, MODEL_DIM), jnp.float32) * MODEL_DIM ** -0.5
    w_up = jax.random.normal(weight_keys[2], (NUM_LAYERS, MODEL_DIM, FFN_DIM), jnp.float32) * MODEL_DIM ** -0.5
    w_down = jax.random.normal(weight_keys[3], (NUM_LAYERS, FFN_DIM, MODEL_DIM), jnp.float32) * FFN_DIM ** -0.5
    gain_one = jax.random.uniform(weight_keys[4], (NUM_LAYERS, MODEL_DIM), jnp.float32, 0.5, 1.5)
    gain_two = jax.random.uniform(weight_keys[5], (NUM_LAYERS, MODEL_DIM), jnp.float32, 0.5, 1.5)
    return {
        "act_in": (shared_mean + token_noise).astype(jnp.bfloat16),
        "w_qkv": w_qkv.astype(jnp.bfloat16),
        "w_out": w_out.astype(jnp.bfloat16),
        "w_up": w_up.astype(jnp.bfloat16),
        "w_down": w_down.astype(jnp.bfloat16),
        "gain_one": gain_one,
        "gain_two": gain_two,
    }


def layer_norm(act_rows, gain_vec):
    rows_f32 = act_rows.astype(jnp.float32)
    centred = rows_f32 - jnp.mean(rows_f32, axis=-1, keepdims=True)
    var_rows = jnp.mean(centred * centred, axis=-1, keepdims=True)
    return (centred * lax.rsqrt(var_rows + 1e-5) * gain_vec).astype(jnp.bfloat16)


def causal_attention(query_rows, key_rows, value_rows):
    key_pos = jnp.arange(SEQ_LEN)
    key_f32 = key_rows.astype(jnp.float32)
    value_f32 = value_rows.astype(jnp.float32)

    def one_block(blk_idx):
        row_start = blk_idx * ROW_BLOCK
        q_blk = lax.dynamic_slice_in_dim(query_rows, row_start, ROW_BLOCK, axis=0).astype(jnp.float32)
        scores = jnp.einsum("qhd,khd->hqk", q_blk, key_f32) * SCORE_SCALE
        q_pos = row_start + jnp.arange(ROW_BLOCK)
        scores = jnp.where(key_pos[None, None, :] <= q_pos[None, :, None], scores, -1e30)
        exp_scores = jnp.exp(scores - jnp.max(scores, axis=-1, keepdims=True))
        prob_sum = jnp.sum(exp_scores, axis=-1)
        mix_out = jnp.einsum("hqk,khd->qhd", exp_scores.astype(jnp.bfloat16).astype(jnp.float32), value_f32)
        return (mix_out / prob_sum.T[:, :, None]).astype(jnp.bfloat16)

    blocks = lax.map(one_block, jnp.arange(SEQ_LEN // ROW_BLOCK))
    return blocks.reshape(SEQ_LEN, NUM_HEADS, HEAD_DIM)


def reference(act_in, w_qkv, w_out, w_up, w_down, gain_one, gain_two):
    def layer_step(act_rows, layer_weights):
        qkv_mat, out_mat, up_mat, down_mat, norm_one, norm_two = layer_weights
        normed = layer_norm(act_rows, norm_one)
        qkv_rows = jnp.dot(normed, qkv_mat.reshape(MODEL_DIM, 3 * MODEL_DIM), preferred_element_type=jnp.float32).astype(jnp.bfloat16)
        qkv_rows = qkv_rows.reshape(SEQ_LEN, NUM_HEADS, 3, HEAD_DIM)
        attn_rows = causal_attention(qkv_rows[:, :, 0], qkv_rows[:, :, 1], qkv_rows[:, :, 2])
        branch = jnp.dot(attn_rows.reshape(SEQ_LEN, MODEL_DIM), out_mat.reshape(MODEL_DIM, MODEL_DIM), preferred_element_type=jnp.float32)
        act_rows = (act_rows.astype(jnp.float32) + branch).astype(jnp.bfloat16)
        normed = layer_norm(act_rows, norm_two)
        hidden = jax.nn.gelu(jnp.dot(normed, up_mat, preferred_element_type=jnp.float32), approximate=True).astype(jnp.bfloat16)
        branch = jnp.dot(hidden, down_mat, preferred_element_type=jnp.float32)
        act_rows = (act_rows.astype(jnp.float32) + branch).astype(jnp.bfloat16)
        return act_rows, None

    final_rows = lax.scan(layer_step, act_in, (w_qkv, w_out, w_up, w_down, gain_one, gain_two))[0]
    return final_rows
```

```python
import functools
import math
import jax
import jax.numpy as jnp
from jax import lax
from jax.experimental import pallas as pl
from jax.experimental.pallas import tpu as pltpu
from jax.sharding import PartitionSpec as P

F32 = jnp.float32
BF16 = jnp.bfloat16
SIDE = 4
CORES = 2
TILES = 8


def norm_rows(rows, gain):
    centred = rows - jnp.mean(rows, axis=-1, keepdims=True)
    var = jnp.mean(centred * centred, axis=-1, keepdims=True)
    return centred * lax.rsqrt(var + 1e-5) * gain


def stack_kernel(act, hq, ho, hu, hd, gains, out,
                 wq, wo, wu, wd, part, psnd, prcv, tb, db, eb, tb2, db2, eb2,
                 kc, vc, ob, hid, xres,
                 wsem, pss, psr, rss, rsr, ags, agr, dds, ddr):
    layers = hq.shape[0]
    rows = act.shape[1] * act.shape[2] * act.shape[3]
    brow = act.shape[3]
    width = act.shape[4]
    head = hq.shape[3]
    tile = width // TILES
    halves = 2 * layers
    slots = CORES * halves
    scale = 1.0 / math.sqrt(head)

    t = lax.axis_index("tp")
    z = lax.axis_index("dp")
    m = lax.rem(t, CORES)
    x = lax.rem(lax.div(t, CORES), SIDE)
    y = lax.div(t, CORES * SIDE)
    partner = t + 1 - 2 * m

    def dev(yy, xx):
        return (yy * SIDE + xx) * CORES + m

    def ring(along_x):
        me = x if along_x else y
        r, o, l = (lax.rem(me + k, SIDE) for k in (1, 2, 3))
        if along_x:
            return me, r, l, o, dev(y, r), dev(y, l)
        return me, r, l, o, dev(r, x), dev(l, x)

    rings = {True: ring(True), False: ring(False)}

    barrier = pltpu.get_barrier_semaphore()
    peers = [partner, rings[True][4], rings[True][5], rings[False][4], rings[False][5]]
    for peer in peers:
        pl.semaphore_signal(barrier, inc=1, device_id=(z, peer), device_id_type=pl.DeviceIdType.MESH)

    def weight_copies(l, kind):
        if kind == 0:
            cps = [pltpu.make_async_copy(
                hq.at[l, c], wq.at[l, :, pl.ds(c * head, head)], wsem.at[l, c]) for c in range(3)]
            return cps + [pltpu.make_async_copy(ho.at[l], wo.at[l], wsem.at[l, 3])]
        return [pltpu.make_async_copy(hu.at[l], wu.at[l], wsem.at[l, 4]),
                pltpu.make_async_copy(hd.at[l], wd.at[l], wsem.at[l, 5])]

    for l in range(layers):
        for kind in range(2):
            for cp in weight_copies(l, kind):
                cp.start()

    kc[...] = jnp.zeros_like(kc)
    vc[...] = jnp.zeros_like(vc)

    def first_norm(i, carry):
        c = lax.div(i, SIDE)
        b = lax.rem(i, SIDE)
        out[c, b] = norm_rows(act[c, b].astype(F32), gains[0]).astype(BF16)
        return carry

    lax.fori_loop(0, CORES * SIDE, first_norm, 0)
    xres[...] = act[m, y, x]

    pl.semaphore_wait(barrier, len(peers))

    def remote(src, dst, ss, rs, peer):
        return pltpu.make_async_remote_copy(
            src_ref=src, dst_ref=dst, send_sem=ss, recv_sem=rs,
            device_id=(z, peer), device_id_type=pl.DeviceIdType.MESH)

    quarter = width // 4

    def cols(o):
        h1 = pl.ds(2 * o * quarter, quarter)
        h2 = pl.ds((2 * o + 1) * quarter, quarter)
        return h1, h2, pl.ds(2 * o * quarter, 2 * quarter)

    def rs_blk(o, ph, b, cs):
        if ph == 0:
            return part.at[:, b, :, cs] if o == 0 else part.at[b, :, :, cs]
        return part.at[b, x, :, cs] if o == 0 else part.at[y, b, :, cs]

    def rs_desc(o, ph, k):
        me, r, l, op, rdev, ldev = rings[(o + ph) % 2 == 0]
        h1, h2, _ = cols(o)
        tt, dd, ee = (tb, db, eb) if ph == 0 else (tb2, db2, eb2)
        b, cs, dst, to = [
            (op, h1, tt.at[o, 0], rdev), (op, h2, tt.at[o, 1], ldev),
            (r, h2, dd.at[o, 0], rdev), (l, h1, dd.at[o, 1], ldev),
            (r, h1, ee.at[o, 0], rdev), (l, h2, ee.at[o, 1], ldev)][k]
        return remote(rs_blk(o, ph, b, cs), dst, rss.at[o, ph, k], rsr.at[o, ph, k], to)

    def rs_start(o, ph):
        for k in range(4):
            rs_desc(o, ph, k).start()

    def rs_fwd(o, ph):
        _, r, l, _, _, _ = rings[(o + ph) % 2 == 0]
        h1, h2, _ = cols(o)
        tt = tb if ph == 0 else tb2
        for k, b, cs in ((0, r, h1), (1, l, h2)):
            rs_desc(o, ph, k).wait_recv()
            blk = rs_blk(o, ph, b, cs)
            blk[...] = (blk[...].astype(F32) + tt[o, k].astype(F32)).astype(BF16)
            rs_desc(o, ph, 4 + k).start()

    def rs_sums(o, ph):
        me = rings[(o + ph) % 2 == 0][0]
        h1, h2, _ = cols(o)
        dd, ee = (db, eb) if ph == 0 else (db2, eb2)
        for k in (2, 3, 4, 5):
            rs_desc(o, ph, k).wait_recv()
        res = []
        for cs, a, b in ((h1, ee.at[o, 0], dd.at[o, 1]), (h2, ee.at[o, 1], dd.at[o, 0])):
            blk = rs_blk(o, ph, me, cs)
            res.append((blk, cs, blk[...].astype(F32) + a[...].astype(F32) + b[...].astype(F32)))
        return res

    def ag_grp(o, ph, b, cs, c):
        if ph == 0:
            return out.at[c, b, x, :, cs] if o == 0 else out.at[c, y, b, :, cs]
        return out.at[c, :, b, :, cs] if o == 0 else out.at[c, b, :, :, cs]

    def ag_desc(o, ph, k):
        me, r, l, op, rdev, ldev = rings[(o + ph) % 2 == 1]
        h1, h2, full = cols(o)
        b, cs, to = [(me, full, rdev), (me, full, ldev), (l, h1, rdev), (r, h2, ldev)][k]
        ref = ag_grp(o, ph, b, cs, m)
        return remote(ref, ref, ags.at[o, ph, k], agr.at[o, ph, k], to)

    def dd_desc(o, k, c):
        me, r, l, op, _, _ = rings[o == 0]
        h1, h2, full = cols(o)
        b, cs = [(me, full), (l, full), (r, full), (op, h1), (op, h2)][k]
        ref = ag_grp(o, 1, b, cs, c)
        return remote(ref, ref, dds.at[o, k], ddr.at[o, k], partner)

    def wait_other():
        for o in range(2):
            for k in range(5):
                dd_desc(o, k, 1 - m).wait_recv()

    def p_desc(n):
        return remote(psnd.at[n], prcv.at[n], pss.at[n], psr.at[n], partner)

    def attention(c, l):
        a = out[c].reshape(rows, width)
        qkv = jnp.dot(a, wq[l], preferred_element_type=F32).astype(BF16)
        base = pl.multiple_of(c * rows, rows)
        kc[pl.ds(base, rows), :] = qkv[:, head:2 * head]
        vc[pl.ds(base, rows), :] = qkv[:, 2 * head:]
        s = lax.dot_general(qkv[:, :head], kc[...], (((1,), (1,)), ((), ())),
                            preferred_element_type=F32) * scale
        q_pos = base + lax.broadcasted_iota(jnp.int32, s.shape, 0)
        k_pos = lax.broadcasted_iota(jnp.int32, s.shape, 1)
        s = jnp.where(k_pos <= q_pos, s, -1e30)
        p = jnp.exp(s - jnp.max(s, axis=-1, keepdims=True))
        mix = jnp.dot(p.astype(BF16), vc[...], preferred_element_type=F32)
        ob[...] = (mix / jnp.sum(p, axis=-1, keepdims=True)).astype(BF16)

    def mlp_up(c, l):
        def body(n, carry):
            cs = pl.ds(pl.multiple_of(n * 256, 256), 256)
            a = out[c].reshape(rows, width)
            up = jnp.dot(a, wu[l, :, cs], preferred_element_type=F32)
            hid[:, cs] = jax.nn.gelu(up, approximate=True).astype(BF16)
            return carry
        lax.fori_loop(0, hid.shape[1] // 256, body, 0)

    def emit_tile(n, acc, own):
        @pl.when(own)
        def _():
            p_desc(n).wait_recv()
            total = (acc + prcv[n].astype(F32)).astype(BF16)
            cs = pl.ds(pl.multiple_of(n * tile, tile), tile)
            part[:, :, :, cs] = total.reshape(SIDE, SIDE, brow, tile)

        @pl.when(jnp.logical_not(own))
        def _():
            psnd[n] = acc.astype(BF16)
            p_desc(n).start()

    def down(o, l, odd, own):
        lo = o * (TILES // 2)

        def body(n, carry, lhs, w):
            cs = pl.ds(pl.multiple_of(n * tile, tile), tile)
            emit_tile(n, jnp.dot(lhs[...], w[l, :, cs], preferred_element_type=F32), own)
            return carry

        @pl.when(odd == 0)
        def _():
            lax.fori_loop(lo, lo + TILES // 2, functools.partial(body, lhs=ob, w=wo), 0)

        @pl.when(odd == 1)
        def _():
            lax.fori_loop(lo, lo + TILES // 2, functools.partial(body, lhs=hid, w=wd), 0)

    def slot(s, carry):
        c = lax.rem(s, CORES)
        h = lax.div(s, CORES)
        l = lax.div(h, 2)
        odd = lax.rem(h, 2)
        own = c == m
        other = c != m

        @pl.when(jnp.logical_and(other, s >= CORES))
        def _():
            wait_other()

        @pl.when(s < slots)
        def _():
            for kind in range(2):
                @pl.when(jnp.logical_and(c == 0, odd == kind))
                def _():
                    for cp in weight_copies(l, kind):
                        cp.wait()

            @pl.when(odd == 0)
            def _():
                attention(c, l)

            @pl.when(odd == 1)
            def _():
                mlp_up(c, l)

            for o in range(2):
                down(o, l, odd, own)

                @pl.when(own)
                def _():
                    rs_start(o, 0)

            @pl.when(own)
            def _():
                for o in range(2):
                    rs_fwd(o, 0)
                for o in range(2):
                    for blk, _, total in rs_sums(o, 0):
                        blk[...] = total.astype(BF16)
                    rs_start(o, 1)
                for o in range(2):
                    rs_fwd(o, 1)

        @pl.when(jnp.logical_and(other, s >= 1))
        def _():
            done = lax.div(s - 1, CORES)
            for o in range(2):
                for _, cs, total in rs_sums(o, 1):
                    xres[:, cs] = (xres[:, cs].astype(F32) + total).astype(BF16)
            xs = xres[...].astype(F32)
            gain = gains[lax.min(done + 1, halves - 1)]
            nrm = norm_rows(xs, gain)
            out[m, y, x] = jnp.where(done == halves - 1, xs, nrm).astype(BF16)
            for o in range(2):
                ag_desc(o, 0, 0).start()
                ag_desc(o, 0, 1).start()
            for o in range(2):
                for k in range(2):
                    ag_desc(o, 0, k).wait_recv()
                    ag_desc(o, 0, 2 + k).start()
            for o in range(2):
                ag_desc(o, 0, 2).wait_recv()
                ag_desc(o, 0, 3).wait_recv()
                ag_desc(o, 1, 0).start()
                ag_desc(o, 1, 1).start()
                dd_desc(o, 0, m).start()
            for o in range(2):
                for k in range(2):
                    ag_desc(o, 1, k).wait_recv()
                    ag_desc(o, 1, 2 + k).start()
                    dd_desc(o, 1 + k, m).start()
            for o in range(2):
                for k in range(2):
                    ag_desc(o, 1, 2 + k).wait_recv()
                    dd_desc(o, 3 + k, m).start()
            for o in range(2):
                for ph in range(2):
                    for k in range(6):
                        rs_desc(o, ph, k).wait_send()
                    for k in range(4):
                        ag_desc(o, ph, k).wait_send()
                for k in range(5):
                    dd_desc(o, k, m).wait_send()

            @pl.when(s < slots)
            def _():
                for n in range(TILES):
                    p_desc(n).wait_send()

        @pl.when(jnp.logical_and(other, s == 0))
        def _():
            for n in range(TILES):
                p_desc(n).wait_send()

        return carry

    lax.fori_loop(0, slots + 1, slot, 0)

    @pl.when(m == 0)
    def _():
        wait_other()


def solution(mesh):
    tp = mesh.shape["tp"]

    def device_fn(act_in, w_qkv, w_out, w_up, w_down, gain_one, gain_two):
        layers, width, _, _, head = w_qkv.shape
        seq = act_in.shape[0]
        ffn = w_up.shape[2]
        rows = seq // CORES
        brow = rows // (SIDE * SIDE)
        assert tp == SIDE * SIDE * CORES
        blocks = (CORES, SIDE, SIDE, brow, width)
        q_view = jnp.transpose(w_qkv, (0, 2, 3, 1, 4)).reshape(layers, 3, width, head)
        gains = jnp.stack([gain_one, gain_two], axis=1).reshape(2 * layers, 1, width)
        quarter = width // 4
        tile = width // TILES
        vmem = pltpu.VMEM
        dma = pltpu.SemaphoreType.DMA
        any_spec = pl.BlockSpec(memory_space=pl.ANY)
        vmem_spec = pl.BlockSpec(memory_space=pltpu.VMEM)
        big = (2, 2, SIDE, brow, quarter)
        small = (2, 2, brow, quarter)
        res = pl.pallas_call(
            stack_kernel,
            out_shape=jax.ShapeDtypeStruct(blocks, BF16),
            in_specs=[vmem_spec, any_spec, any_spec, any_spec, any_spec, vmem_spec],
            out_specs=vmem_spec,
            scratch_shapes=[
                vmem((layers, width, 3 * head), BF16),
                vmem((layers, head, width), BF16),
                vmem((layers, width, ffn), BF16),
                vmem((layers, ffn, width), BF16),
                vmem((SIDE, SIDE, brow, width), BF16),
                vmem((TILES, rows, tile), BF16),
                vmem((TILES, rows, tile), BF16),
                vmem(big, BF16), vmem(big, BF16), vmem(big, BF16),
                vmem(small, BF16), vmem(small, BF16), vmem(small, BF16),
                vmem((seq, head), BF16), vmem((seq, head), BF16),
                vmem((rows, head), BF16), vmem((rows, ffn), BF16),
                vmem((brow, width), BF16),
                dma((layers, 6)),
                dma((TILES,)), dma((TILES,)),
                dma((2, 2, 6)), dma((2, 2, 6)),
                dma((2, 2, 4)), dma((2, 2, 4)),
                dma((2, 5)), dma((2, 5)),
            ],
            compiler_params=pltpu.CompilerParams(
                collective_id=0, has_side_effects=True, vmem_limit_bytes=63 * 2 ** 20),
            name="layer_stack",
        )(act_in.reshape(blocks), q_view, w_out.reshape(layers, head, width), w_up, w_down, gains)
        return res.reshape(seq, width)

    return jax.shard_map(
        device_fn,
        mesh=mesh,
        in_specs=(
            P("dp", None),
            P(None, None, "tp", None, None),
            P(None, "tp", None, None),
            P(None, None, "tp"),
            P(None, "tp", None),
            P(None, None),
            P(None, None),
        ),
        out_specs=P("dp", None),
        check_vma=False,
    )
```

```python
import functools
import math
import jax
import jax.numpy as jnp
from jax import lax
from jax.experimental import pallas as pl
from jax.experimental.pallas import tpu as pltpu
from jax.sharding import PartitionSpec as P

F32 = jnp.float32
BF16 = jnp.bfloat16
SIDE = 4
CORES = 2
TILES = 8


def norm_rows(rows, gain):
    centred = rows - jnp.mean(rows, axis=-1, keepdims=True)
    var = jnp.mean(centred * centred, axis=-1, keepdims=True)
    return centred * lax.rsqrt(var + 1e-5) * gain


def stack_kernel(act, hq, ho, hu, hd, gains, out,
                 wq, wo, wu, wd, part, psnd, prcv, tb, db, eb, tb2, db2, eb2,
                 kc, vc, ob, hid, xres,
                 wsem, pss, psr, rss, rsr, ags, agr, dds, ddr):
    layers = hq.shape[0]
    rows = act.shape[1] * act.shape[2] * act.shape[3]
    brow = act.shape[3]
    width = act.shape[4]
    head = hq.shape[3]
    tile = width // TILES
    halves = 2 * layers
    slots = CORES * halves
    scale = 1.0 / math.sqrt(head)

    t = lax.axis_index("tp")
    z = lax.axis_index("dp")
    m = lax.rem(t, CORES)
    x = lax.rem(lax.div(t, CORES), SIDE)
    y = lax.div(t, CORES * SIDE)
    partner = t + 1 - 2 * m

    def dev(yy, xx):
        return (yy * SIDE + xx) * CORES + m

    def ring(along_x):
        me = x if along_x else y
        r, o, l = (lax.rem(me + k, SIDE) for k in (1, 2, 3))
        if along_x:
            return me, r, l, o, dev(y, r), dev(y, l)
        return me, r, l, o, dev(r, x), dev(l, x)

    rings = {True: ring(True), False: ring(False)}

    barrier = pltpu.get_barrier_semaphore()
    peers = [partner, rings[True][4], rings[True][5], rings[False][4], rings[False][5]]
    for peer in peers:
        pl.semaphore_signal(barrier, inc=1, device_id=(z, peer), device_id_type=pl.DeviceIdType.MESH)

    def weight_copies(l, kind):
        if kind == 0:
            cps = [pltpu.make_async_copy(
                hq.at[l, c], wq.at[l, :, pl.ds(c * head, head)], wsem.at[l, c]) for c in range(3)]
            return cps + [pltpu.make_async_copy(ho.at[l], wo.at[l], wsem.at[l, 3])]
        return [pltpu.make_async_copy(hu.at[l], wu.at[l], wsem.at[l, 4]),
                pltpu.make_async_copy(hd.at[l], wd.at[l], wsem.at[l, 5])]

    for l in range(layers):
        for kind in range(2):
            for cp in weight_copies(l, kind):
                cp.start()

    kc[...] = jnp.zeros_like(kc)
    vc[...] = jnp.zeros_like(vc)

    def first_norm(i, carry):
        c = lax.div(i, SIDE)
        b = lax.rem(i, SIDE)
        out[c, b] = norm_rows(act[c, b].astype(F32), gains[0]).astype(BF16)
        return carry

    with jax.named_scope("first_norm"):
        lax.fori_loop(0, CORES * SIDE, first_norm, 0)
    xres[...] = act[m, y, x]

    pl.semaphore_wait(barrier, len(peers))

    def remote(src, dst, ss, rs, peer):
        return pltpu.make_async_remote_copy(
            src_ref=src, dst_ref=dst, send_sem=ss, recv_sem=rs,
            device_id=(z, peer), device_id_type=pl.DeviceIdType.MESH)

    quarter = width // 4

    def cols(o):
        h1 = pl.ds(2 * o * quarter, quarter)
        h2 = pl.ds((2 * o + 1) * quarter, quarter)
        return h1, h2, pl.ds(2 * o * quarter, 2 * quarter)

    first = [rings[True], rings[False]]
    second = [rings[False], rings[True]]

    def b2_of(o, p):
        me2, r2, l2, op2, _, _ = second[o]
        return (op2, r2, l2, me2)[p]

    def rs_blk(o, b1, b2, cs):
        return part.at[b2, b1, :, cs] if o == 0 else part.at[b1, b2, :, cs]

    def rs1(o, p, k):
        _, r, l, op, rdev, ldev = first[o]
        h1, h2, _ = cols(o)
        b, cs, dst, to = [
            (op, h1, tb.at[o, 0, p], rdev), (op, h2, tb.at[o, 1, p], ldev),
            (r, h2, db.at[o, 0, p], rdev), (l, h1, db.at[o, 1, p], ldev),
            (r, h1, eb.at[o, 0, p], rdev), (l, h2, eb.at[o, 1, p], ldev)][k]
        return remote(rs_blk(o, b, b2_of(o, p), cs), dst, rss.at[o, p, k], rsr.at[o, p, k], to)

    def rs2(o, k):
        me1 = first[o][0]
        _, r, l, op, rdev, ldev = second[o]
        h1, h2, _ = cols(o)
        b, cs, dst, to = [
            (op, h1, tb2.at[o, 0], rdev), (op, h2, tb2.at[o, 1], ldev),
            (r, h2, db2.at[o, 0], rdev), (l, h1, db2.at[o, 1], ldev),
            (r, h1, eb2.at[o, 0], rdev), (l, h2, eb2.at[o, 1], ldev)][k]
        return remote(rs_blk(o, me1, b, cs), dst, rss.at[o, 4, k], rsr.at[o, 4, k], to)

    def add_to(blk, *others):
        total = blk[...].astype(F32)
        for other in others:
            total = total + other[...].astype(F32)
        return total

    def rs1_start(o):
        for ks in ((0, 1), (2, 3)):
            for p in range(SIDE):
                for k in ks:
                    rs1(o, p, k).start()

    def rs1_forward(o, p):
        _, r, l, _, _, _ = first[o]
        h1, h2, _ = cols(o)
        for k, b, cs in ((0, r, h1), (1, l, h2)):
            rs1(o, p, k).wait_recv()
            blk = rs_blk(o, b, b2_of(o, p), cs)
            blk[...] = add_to(blk, tb.at[o, k, p]).astype(BF16)
            rs1(o, p, 4 + k).start()

    def rs1_sum(o, p):
        h1, h2, _ = cols(o)
        for k in (2, 3, 4, 5):
            rs1(o, p, k).wait_recv()
        for cs, a, b in ((h1, eb.at[o, 0, p], db.at[o, 1, p]), (h2, eb.at[o, 1, p], db.at[o, 0, p])):
            blk = rs_blk(o, first[o][0], b2_of(o, p), cs)
            blk[...] = add_to(blk, a, b).astype(BF16)
        for k in ((0, 1), (2,), (3,), ())[p]:
            rs2(o, k).start()

    def rs2_forward(o):
        _, r, l, _, _, _ = second[o]
        h1, h2, _ = cols(o)
        for k, b, cs in ((0, r, h1), (1, l, h2)):
            rs2(o, k).wait_recv()
            blk = rs_blk(o, first[o][0], b, cs)
            blk[...] = add_to(blk, tb2.at[o, k]).astype(BF16)
            rs2(o, 4 + k).start()

    def rs2_sum(o):
        h1, h2, _ = cols(o)
        for k in (2, 3, 4, 5):
            rs2(o, k).wait_recv()
        for cs, a, b in ((h1, eb2.at[o, 0], db2.at[o, 1]), (h2, eb2.at[o, 1], db2.at[o, 0])):
            blk = rs_blk(o, first[o][0], second[o][0], cs)
            xres[:, cs] = add_to(xres.at[:, cs], blk, a, b).astype(BF16)

    def ag_blk(o, b1, b2, cs):
        return out.at[m, b2, b1, :, cs] if o == 0 else out.at[m, b1, b2, :, cs]

    def ag1(o, k):
        me1 = first[o][0]
        me, r, l, _, rdev, ldev = second[o]
        h1, h2, full = cols(o)
        b, cs, to = [(me, full, rdev), (me, full, ldev), (l, h1, rdev), (r, h2, ldev)][k]
        ref = ag_blk(o, me1, b, cs)
        return remote(ref, ref, ags.at[o, 4, k], agr.at[o, 4, k], to)

    def ag2(o, p, k):
        me, r, l, _, rdev, ldev = first[o]
        h1, h2, full = cols(o)
        b, cs, to = [(me, full, rdev), (me, full, ldev), (l, h1, rdev), (r, h2, ldev)][k]
        ref = ag_blk(o, b, b2_of(o, p), cs)
        return remote(ref, ref, ags.at[o, p, k], agr.at[o, p, k], to)

    def to_partner(o, k, p):
        me, r, l, op, _, _ = first[o]
        h1, h2, full = cols(o)
        b, cs = [(me, full), (l, full), (r, full), (op, h1), (op, h2)][k]
        ref = ag_blk(o, b, b2_of(o, p), cs)
        remote(ref, ref, dds.at[0], ddr.at[0], partner).start()

    def whole(c):
        return remote(out.at[c], out.at[c], dds.at[0], ddr.at[0], partner)

    def wait_other():
        whole(1 - m).wait_recv()

    def gather_piece(o, p):
        ag2(o, p, 0).start()
        ag2(o, p, 1).start()
        to_partner(o, 0, p)

    def gather_forward(o, p):
        for k in range(2):
            ag2(o, p, k).wait_recv()
            ag2(o, p, 2 + k).start()
            to_partner(o, 1 + k, p)

    def gather_end(o, p):
        for k in range(2):
            ag2(o, p, 2 + k).wait_recv()
            to_partner(o, 3 + k, p)

    def p_desc(n):
        return remote(psnd.at[n], prcv.at[n], pss.at[n], psr.at[n], partner)

    def attention(c, l):
        a = out[c].reshape(rows, width)
        qkv = jnp.dot(a, wq[l], preferred_element_type=F32).astype(BF16)
        base = pl.multiple_of(c * rows, rows)
        kc[pl.ds(base, rows), :] = qkv[:, head:2 * head]
        vc[pl.ds(base, rows), :] = qkv[:, 2 * head:]
        s = lax.dot_general(qkv[:, :head], kc[...], (((1,), (1,)), ((), ())),
                            preferred_element_type=F32) * scale
        q_pos = base + lax.broadcasted_iota(jnp.int32, s.shape, 0)
        k_pos = lax.broadcasted_iota(jnp.int32, s.shape, 1)
        s = jnp.where(k_pos <= q_pos, s, -1e30)
        p = jnp.exp(s - jnp.max(s, axis=-1, keepdims=True))
        mix = jnp.dot(p.astype(BF16), vc[...], preferred_element_type=F32)
        ob[...] = (mix / jnp.sum(p, axis=-1, keepdims=True)).astype(BF16)

    def mlp_up(c, l):
        def body(n, carry):
            cs = pl.ds(pl.multiple_of(n * 256, 256), 256)
            a = out[c].reshape(rows, width)
            up = jnp.dot(a, wu[l, :, cs], preferred_element_type=F32)
            hid[:, cs] = jax.nn.gelu(up, approximate=True).astype(BF16)
            return carry
        lax.fori_loop(0, hid.shape[1] // 256, body, 0)

    def emit_tile(n, acc, own):
        @pl.when(own)
        def _():
            p_desc(n).wait_recv()
            total = (acc + prcv[n].astype(F32)).astype(BF16)
            cs = pl.ds(pl.multiple_of(n * tile, tile), tile)
            part[:, :, :, cs] = total.reshape(SIDE, SIDE, brow, tile)

        @pl.when(jnp.logical_not(own))
        def _():
            psnd[n] = acc.astype(BF16)
            p_desc(n).start()

    def down(o, l, odd, own):
        lo = o * (TILES // 2)

        def body(n, carry, lhs, w):
            cs = pl.ds(pl.multiple_of(n * tile, tile), tile)
            emit_tile(n, jnp.dot(lhs[...], w[l, :, cs], preferred_element_type=F32), own)
            return carry

        @pl.when(odd == 0)
        def _():
            lax.fori_loop(lo, lo + TILES // 2, functools.partial(body, lhs=ob, w=wo), 0)

        @pl.when(odd == 1)
        def _():
            lax.fori_loop(lo, lo + TILES // 2, functools.partial(body, lhs=hid, w=wd), 0)

    def scatter_first():
        with jax.named_scope("rs1"):
            for p in range(2):
                for o in range(2):
                    rs1_forward(o, p)
            for p in range(2, SIDE):
                for o in range(2):
                    rs1_sum(o, p - 2)
                    rs1_forward(o, p)
        with jax.named_scope("rs1_end"):
            for p in (2, 3):
                for o in range(2):
                    rs1_sum(o, p)

    def owned_norm(done):
        with jax.named_scope("rs2_sum"):
            for o in range(2):
                rs2_sum(o)
        with jax.named_scope("owned_norm"):
            xs = xres[...].astype(F32)
            gain = gains[lax.min(done + 1, halves - 1)]
            nrm = norm_rows(xs, gain)
            out[m, y, x] = jnp.where(done == halves - 1, xs, nrm).astype(BF16)

    def gather():
        both = range(2)
        with jax.named_scope("ag1"):
            for o in both:
                ag1(o, 0).start()
                ag1(o, 1).start()
            for o in both:
                gather_piece(o, 3)
            for k in range(2):
                for o in both:
                    ag1(o, k).wait_recv()
                    ag1(o, 2 + k).start()
                    gather_piece(o, 2 - k)
        with jax.named_scope("ag2_me"):
            for o in both:
                gather_forward(o, 3)
        with jax.named_scope("ag1_end"):
            for o in both:
                ag1(o, 2).wait_recv()
                ag1(o, 3).wait_recv()
                gather_piece(o, 0)
        with jax.named_scope("ag2_side"):
            for p in (2, 1):
                for o in both:
                    gather_forward(o, p)
        with jax.named_scope("ag2_me_end"):
            for o in both:
                gather_end(o, 3)
        with jax.named_scope("ag2_op"):
            for o in both:
                gather_forward(o, 0)
        with jax.named_scope("ag2_end"):
            for p in (2, 1, 0):
                for o in both:
                    gather_end(o, p)

    def drain():
        with jax.named_scope("drain"):
            for o in range(2):
                for p in range(SIDE):
                    for k in range(6):
                        rs1(o, p, k).wait_send()
                    for k in range(4):
                        ag2(o, p, k).wait_send()
                for k in range(6):
                    rs2(o, k).wait_send()
                for k in range(4):
                    ag1(o, k).wait_send()
            whole(m).wait_send()

    def slot(s, carry):
        c = lax.rem(s, CORES)
        h = lax.div(s, CORES)
        l = lax.div(h, 2)
        odd = lax.rem(h, 2)
        own = c == m
        other = c != m
        closing = jnp.logical_and(other, s >= 1)
        inside = s < slots

        @pl.when(jnp.logical_and(other, s >= CORES))
        def _():
            with jax.named_scope("wait_other"):
                wait_other()

        for kind in range(2):
            @pl.when(jnp.logical_and(inside, odd == kind))
            def _():
                @pl.when(c == 0)
                def _():
                    for cp in weight_copies(l, kind):
                        cp.wait()

                with jax.named_scope("up"):
                    (attention, mlp_up)[kind](c, l)

        @pl.when(closing)
        def _():
            with jax.named_scope("rs2_forward"):
                for o in range(2):
                    rs2_forward(o)

        for o in range(2):
            @pl.when(inside)
            def _():
                with jax.named_scope("down"):
                    down(o, l, odd, own)

            @pl.when(jnp.logical_and(inside, own))
            def _():
                rs1_start(o)

        @pl.when(jnp.logical_and(inside, own))
        def _():
            scatter_first()

        @pl.when(closing)
        def _():
            owned_norm(lax.div(s - 1, CORES))
            gather()
            drain()

        @pl.when(jnp.logical_and(inside, other))
        def _():
            for n in range(TILES):
                p_desc(n).wait_send()

        return carry

    lax.fori_loop(0, slots + 1, slot, 0)

    @pl.when(m == 0)
    def _():
        wait_other()


def solution(mesh):
    tp = mesh.shape["tp"]

    def device_fn(act_in, w_qkv, w_out, w_up, w_down, gain_one, gain_two):
        layers, width, _, _, head = w_qkv.shape
        seq = act_in.shape[0]
        ffn = w_up.shape[2]
        rows = seq // CORES
        brow = rows // (SIDE * SIDE)
        assert tp == SIDE * SIDE * CORES
        blocks = (CORES, SIDE, SIDE, brow, width)
        q_view = jnp.transpose(w_qkv, (0, 2, 3, 1, 4)).reshape(layers, 3, width, head)
        gains = jnp.stack([gain_one, gain_two], axis=1).reshape(2 * layers, 1, width)
        quarter = width // 4
        tile = width // TILES
        vmem = pltpu.VMEM
        dma = pltpu.SemaphoreType.DMA
        any_spec = pl.BlockSpec(memory_space=pl.ANY)
        vmem_spec = pl.BlockSpec(memory_space=pltpu.VMEM)
        big = (2, 2, SIDE, brow, quarter)
        small = (2, 2, brow, quarter)
        res = pl.pallas_call(
            stack_kernel,
            out_shape=jax.ShapeDtypeStruct(blocks, BF16),
            in_specs=[vmem_spec, any_spec, any_spec, any_spec, any_spec, vmem_spec],
            out_specs=vmem_spec,
            scratch_shapes=[
                vmem((layers, width, 3 * head), BF16),
                vmem((layers, head, width), BF16),
                vmem((layers, width, ffn), BF16),
                vmem((layers, ffn, width), BF16),
                vmem((SIDE, SIDE, brow, width), BF16),
                vmem((TILES, rows, tile), BF16),
                vmem((TILES, rows, tile), BF16),
                vmem(big, BF16), vmem(big, BF16), vmem(big, BF16),
                vmem(small, BF16), vmem(small, BF16), vmem(small, BF16),
                vmem((seq, head), BF16), vmem((seq, head), BF16),
                vmem((rows, head), BF16), vmem((rows, ffn), BF16),
                vmem((brow, width), BF16),
                dma((layers, 6)),
                dma((TILES,)), dma((TILES,)),
                dma((2, SIDE + 1, 6)), dma((2, SIDE + 1, 6)),
                dma((2, SIDE + 1, 4)), dma((2, SIDE + 1, 4)),
                dma((1,)), dma((1,)),
            ],
            compiler_params=pltpu.CompilerParams(
                collective_id=0, has_side_effects=True, vmem_limit_bytes=63 * 2 ** 20),
            name="layer_stack",
        )(act_in.reshape(blocks), q_view, w_out.reshape(layers, head, width), w_up, w_down, gains)
        return res.reshape(seq, width)

    return jax.shard_map(
        device_fn,
        mesh=mesh,
        in_specs=(
            P("dp", None),
            P(None, None, "tp", None, None),
            P(None, "tp", None, None),
            P(None, None, "tp"),
            P(None, "tp", None),
            P(None, None),
            P(None, None),
        ),
        out_specs=P("dp", None),
        check_vma=False,
    )
```

```python
import functools
import math
import jax
import jax.numpy as jnp
from jax import lax
from jax.experimental import pallas as pl
from jax.experimental.pallas import tpu as pltpu
from jax.sharding import PartitionSpec as P

F32 = jnp.float32
BF16 = jnp.bfloat16
SIDE = 4
CORES = 2
TILES = 8


def norm_rows(rows, gain):
    centred = rows - jnp.mean(rows, axis=-1, keepdims=True)
    var = jnp.mean(centred * centred, axis=-1, keepdims=True)
    return centred * lax.rsqrt(var + 1e-5) * gain


def stack_kernel(act, hq, ho, hu, hd, gains, out,
                 wq, wo, wu, wd, part, psnd, prcv, fb, gb,
                 kc, vc, ob, hid, xres,
                 wsem, pss, psr, rss, rsr, ags, agr, dds, ddr):
    layers = hq.shape[0]
    rows = act.shape[1] * act.shape[2] * act.shape[3]
    brow = act.shape[3]
    width = act.shape[4]
    head = hq.shape[3]
    tile = width // TILES
    halves = 2 * layers
    slots = CORES * halves
    scale = 1.0 / math.sqrt(head)

    t = lax.axis_index("tp")
    z = lax.axis_index("dp")
    m = lax.rem(t, CORES)
    x = lax.rem(lax.div(t, CORES), SIDE)
    y = lax.div(t, CORES * SIDE)
    partner = t + 1 - 2 * m

    def dev(yy, xx):
        return (yy * SIDE + xx) * CORES + m

    def ring(along_x):
        me = x if along_x else y
        r, o, l = (lax.rem(me + k, SIDE) for k in (1, 2, 3))
        if along_x:
            return me, r, l, o, dev(y, r), dev(y, l), dev(y, o)
        return me, r, l, o, dev(r, x), dev(l, x), dev(o, x)

    rings = {True: ring(True), False: ring(False)}

    barrier = pltpu.get_barrier_semaphore()
    peers = [partner, *rings[True][4:], *rings[False][4:]]
    for peer in peers:
        pl.semaphore_signal(barrier, inc=1, device_id=(z, peer), device_id_type=pl.DeviceIdType.MESH)

    def weight_copies(l, kind):
        if kind == 0:
            cps = [pltpu.make_async_copy(
                hq.at[l, c], wq.at[l, :, pl.ds(c * head, head)], wsem.at[l, c]) for c in range(3)]
            return cps + [pltpu.make_async_copy(ho.at[l], wo.at[l], wsem.at[l, 3])]
        return [pltpu.make_async_copy(hu.at[l], wu.at[l], wsem.at[l, 4]),
                pltpu.make_async_copy(hd.at[l], wd.at[l], wsem.at[l, 5])]

    for l in range(layers):
        for kind in range(2):
            for cp in weight_copies(l, kind):
                cp.start()

    kc[...] = jnp.zeros_like(kc)
    vc[...] = jnp.zeros_like(vc)

    def first_norm(i, carry):
        c = lax.div(i, SIDE)
        b = lax.rem(i, SIDE)
        out[c, b] = norm_rows(act[c, b].astype(F32), gains[0]).astype(BF16)
        return carry

    with jax.named_scope("first_norm"):
        lax.fori_loop(0, CORES * SIDE, first_norm, 0)
    xres[...] = act[m, y, x]

    pl.semaphore_wait(barrier, len(peers))

    def remote(src, dst, ss, rs, peer):
        return pltpu.make_async_remote_copy(
            src_ref=src, dst_ref=dst, send_sem=ss, recv_sem=rs,
            device_id=(z, peer), device_id_type=pl.DeviceIdType.MESH)

    half = width // 2

    def cols(o):
        return pl.ds(o * half, half)

    first = [rings[True], rings[False]]
    second = [rings[False], rings[True]]

    def b2_of(o, p):
        me2, r2, l2, op2 = second[o][:4]
        return (op2, r2, l2, me2)[p]

    def rs_blk(o, b1, b2, cs):
        return part.at[b2, b1, :, cs] if o == 0 else part.at[b1, b2, :, cs]

    def rs1(o, p, k):
        _, r, l, op, rdev, ldev, opdev = first[o]
        b, to = [(op, opdev), (r, rdev), (l, ldev)][k]
        src = rs_blk(o, b, b2_of(o, p), cols(o))
        return remote(src, fb.at[o, k, p], rss.at[o, p, k], rsr.at[o, p, k], to)

    def rs2(o, k):
        _, r, l, op, rdev, ldev, opdev = second[o]
        b, to = [(op, opdev), (r, rdev), (l, ldev)][k]
        return remote(rs_blk(o, first[o][0], b, cols(o)), gb.at[o, k], rss.at[o, 4, k], rsr.at[o, 4, k], to)

    def add_to(blk, *others):
        total = blk[...].astype(F32)
        for other in others:
            total = total + other[...].astype(F32)
        return total

    def rs1_start(o):
        for p in range(SIDE):
            for k in range(3):
                rs1(o, p, k).start()

    def rs1_sum(o, p):
        for k in range(3):
            rs1(o, p, k).wait_recv()
        blk = rs_blk(o, first[o][0], b2_of(o, p), cols(o))
        blk[...] = add_to(blk, *(fb.at[o, k, p] for k in range(3))).astype(BF16)
        if p < 3:
            rs2(o, p).start()

    def rs2_sum(o):
        full = cols(o)
        for k in range(3):
            rs2(o, k).wait_recv()
        blk = rs_blk(o, first[o][0], second[o][0], full)
        xres[:, full] = add_to(xres.at[:, full], blk, *(gb.at[o, k] for k in range(3))).astype(BF16)

    def ag_blk(o, b1, b2, cs):
        return out.at[m, b2, b1, :, cs] if o == 0 else out.at[m, b1, b2, :, cs]

    def ag1(o, k):
        to = second[o][4 + (2, 0, 1)[k]]
        ref = ag_blk(o, first[o][0], second[o][0], cols(o))
        return remote(ref, ref, ags.at[o, 4, k], agr.at[o, 4, k], to)

    def ag2(o, p, k):
        to = first[o][4 + (2, 0, 1)[k]]
        ref = ag_blk(o, first[o][0], b2_of(o, p), cols(o))
        return remote(ref, ref, ags.at[o, p, k], agr.at[o, p, k], to)

    def to_partner(o, b, p):
        ref = ag_blk(o, b, b2_of(o, p), cols(o))
        remote(ref, ref, dds.at[0], ddr.at[0], partner).start()

    def whole(c):
        return remote(out.at[c], out.at[c], dds.at[0], ddr.at[0], partner)

    def wait_other():
        whole(1 - m).wait_recv()

    def gather_piece(o, p):
        for k in range(3):
            ag2(o, p, k).start()
        to_partner(o, first[o][0], p)

    def p_desc(n):
        return remote(psnd.at[n], prcv.at[n], pss.at[n], psr.at[n], partner)

    def attention(c, l):
        a = out[c].reshape(rows, width)
        qkv = jnp.dot(a, wq[l], preferred_element_type=F32).astype(BF16)
        base = pl.multiple_of(c * rows, rows)
        kc[pl.ds(base, rows), :] = qkv[:, head:2 * head]
        vc[pl.ds(base, rows), :] = qkv[:, 2 * head:]
        s = lax.dot_general(qkv[:, :head], kc[...], (((1,), (1,)), ((), ())),
                            preferred_element_type=F32) * scale
        q_pos = base + lax.broadcasted_iota(jnp.int32, s.shape, 0)
        k_pos = lax.broadcasted_iota(jnp.int32, s.shape, 1)
        s = jnp.where(k_pos <= q_pos, s, -1e30)
        p = jnp.exp(s - jnp.max(s, axis=-1, keepdims=True))
        mix = jnp.dot(p.astype(BF16), vc[...], preferred_element_type=F32)
        ob[...] = (mix / jnp.sum(p, axis=-1, keepdims=True)).astype(BF16)

    def mlp_up(c, l):
        def body(n, carry):
            cs = pl.ds(pl.multiple_of(n * 256, 256), 256)
            a = out[c].reshape(rows, width)
            up = jnp.dot(a, wu[l, :, cs], preferred_element_type=F32)
            hid[:, cs] = jax.nn.gelu(up, approximate=True).astype(BF16)
            return carry
        lax.fori_loop(0, hid.shape[1] // 256, body, 0)

    def emit_tile(n, acc, own):
        @pl.when(own)
        def _():
            p_desc(n).wait_recv()
            total = (acc + prcv[n].astype(F32)).astype(BF16)
            cs = pl.ds(pl.multiple_of(n * tile, tile), tile)
            part[:, :, :, cs] = total.reshape(SIDE, SIDE, brow, tile)

        @pl.when(jnp.logical_not(own))
        def _():
            psnd[n] = acc.astype(BF16)
            p_desc(n).start()

    def down(o, l, odd, own):
        lo = o * (TILES // 2)

        def body(n, carry, lhs, w):
            cs = pl.ds(pl.multiple_of(n * tile, tile), tile)
            emit_tile(n, jnp.dot(lhs[...], w[l, :, cs], preferred_element_type=F32), own)
            return carry

        @pl.when(odd == 0)
        def _():
            lax.fori_loop(lo, lo + TILES // 2, functools.partial(body, lhs=ob, w=wo), 0)

        @pl.when(odd == 1)
        def _():
            lax.fori_loop(lo, lo + TILES // 2, functools.partial(body, lhs=hid, w=wd), 0)

    def reduce_and_norm(done):
        for p in range(SIDE):
            with jax.named_scope(f"rs1_sum{p}"):
                for o in range(2):
                    rs1_sum(o, p)
        with jax.named_scope("rs2_sum"):
            for o in range(2):
                rs2_sum(o)
        with jax.named_scope("owned_norm"):
            xs = xres[...].astype(F32)
            gain = gains[lax.min(done + 1, halves - 1)]
            nrm = norm_rows(xs, gain)
            out[m, y, x] = jnp.where(done == halves - 1, xs, nrm).astype(BF16)

    def gather_start():
        with jax.named_scope("ag1"):
            for k in range(3):
                for o in range(2):
                    ag1(o, k).start()
            for o in range(2):
                gather_piece(o, 3)
        for k in (1, 2, 0):
            with jax.named_scope(f"ag1_{k}"):
                for o in range(2):
                    ag1(o, k).wait_recv()
                    gather_piece(o, (0, 2, 1)[k])

    def gather_end():
        for p in (3, 2, 1, 0):
            with jax.named_scope(f"ag2_{p}"):
                for o in range(2):
                    for k in range(3):
                        ag2(o, p, k).wait_recv()
                        to_partner(o, first[o][(3, 2, 1)[k]], p)

    def drain():
        with jax.named_scope("drain"):
            for o in range(2):
                for k in range(3):
                    for p in range(SIDE):
                        rs1(o, p, k).wait_send()
                        ag2(o, p, k).wait_send()
                    rs2(o, k).wait_send()
                    ag1(o, k).wait_send()
            whole(m).wait_send()

    def slot(s, carry):
        c = lax.rem(s, CORES)
        h = lax.div(s, CORES)
        l = lax.div(h, 2)
        odd = lax.rem(h, 2)
        own = c == m
        other = c != m
        inside = s < slots

        @pl.when(jnp.logical_and(other, s >= CORES))
        def _():
            with jax.named_scope("wait_other"):
                wait_other()

        for kind in range(2):
            @pl.when(jnp.logical_and(inside, odd == kind))
            def _():
                @pl.when(c == 0)
                def _():
                    for cp in weight_copies(l, kind):
                        cp.wait()

                with jax.named_scope("up"):
                    (attention, mlp_up)[kind](c, l)

        @pl.when(jnp.logical_and(jnp.logical_and(inside, own), s >= CORES))
        def _():
            drain()

        for o in range(2):
            @pl.when(inside)
            def _():
                with jax.named_scope("down"):
                    down(o, l, odd, own)

            @pl.when(jnp.logical_and(inside, own))
            def _():
                rs1_start(o)

        @pl.when(c == 1)
        def _():
            reduce_and_norm(h)
            gather_start()

        @pl.when(jnp.logical_and(s >= 1, other))
        def _():
            gather_end()

        @pl.when(jnp.logical_and(inside, other))
        def _():
            for n in range(TILES):
                p_desc(n).wait_send()

        return carry

    lax.fori_loop(0, slots + 1, slot, 0)
    drain()

    @pl.when(m == 0)
    def _():
        wait_other()


def solution(mesh):
    tp = mesh.shape["tp"]

    def device_fn(act_in, w_qkv, w_out, w_up, w_down, gain_one, gain_two):
        layers, width, _, _, head = w_qkv.shape
        seq = act_in.shape[0]
        ffn = w_up.shape[2]
        rows = seq // CORES
        brow = rows // (SIDE * SIDE)
        assert tp == SIDE * SIDE * CORES
        blocks = (CORES, SIDE, SIDE, brow, width)
        q_view = jnp.transpose(w_qkv, (0, 2, 3, 1, 4)).reshape(layers, 3, width, head)
        gains = jnp.stack([gain_one, gain_two], axis=1).reshape(2 * layers, 1, width)
        half = width // 2
        tile = width // TILES
        vmem = pltpu.VMEM
        dma = pltpu.SemaphoreType.DMA
        any_spec = pl.BlockSpec(memory_space=pl.ANY)
        vmem_spec = pl.BlockSpec(memory_space=pltpu.VMEM)
        res = pl.pallas_call(
            stack_kernel,
            out_shape=jax.ShapeDtypeStruct(blocks, BF16),
            in_specs=[vmem_spec, any_spec, any_spec, any_spec, any_spec, vmem_spec],
            out_specs=vmem_spec,
            scratch_shapes=[
                vmem((layers, width, 3 * head), BF16),
                vmem((layers, head, width), BF16),
                vmem((layers, width, ffn), BF16),
                vmem((layers, ffn, width), BF16),
                vmem((SIDE, SIDE, brow, width), BF16),
                vmem((TILES, rows, tile), BF16),
                vmem((TILES, rows, tile), BF16),
                vmem((2, 3, SIDE, brow, half), BF16),
                vmem((2, 3, brow, half), BF16),
                vmem((seq, head), BF16), vmem((seq, head), BF16),
                vmem((rows, head), BF16), vmem((rows, ffn), BF16),
                vmem((brow, width), BF16),
                dma((layers, 6)),
                dma((TILES,)), dma((TILES,)),
                dma((2, SIDE + 1, 3)), dma((2, SIDE + 1, 3)),
                dma((2, SIDE + 1, 3)), dma((2, SIDE + 1, 3)),
                dma((1,)), dma((1,)),
            ],
            compiler_params=pltpu.CompilerParams(
                collective_id=0, has_side_effects=True, vmem_limit_bytes=63 * 2 ** 20),
            name="layer_stack",
        )(act_in.reshape(blocks), q_view, w_out.reshape(layers, head, width), w_up, w_down, gains)
        return res.reshape(seq, width)

    return jax.shard_map(
        device_fn,
        mesh=mesh,
        in_specs=(
            P("dp", None),
            P(None, None, "tp", None, None),
            P(None, "tp", None, None),
            P(None, None, "tp"),
            P(None, "tp", None),
            P(None, None),
            P(None, None),
        ),
        out_specs=P("dp", None),
        check_vma=False,
    )
```

```python
import functools
import math
import jax
import jax.numpy as jnp
from jax import lax
from jax.experimental import pallas as pl
from jax.experimental.pallas import tpu as pltpu
from jax.sharding import PartitionSpec as P

F32 = jnp.float32
BF16 = jnp.bfloat16
SIDE = 4
CORES = 2
TILES = 8


def norm_rows(rows, gain):
    centred = rows - jnp.mean(rows, axis=-1, keepdims=True)
    var = jnp.mean(centred * centred, axis=-1, keepdims=True)
    return centred * lax.rsqrt(var + 1e-5) * gain


def stack_kernel(act, hq, ho, hu, hd, gain1, gain2, out,
                 wq, wo, wu, wd, part, psnd, prcv, fb, gb,
                 kc, vc, ob, hid, xres,
                 asem, wsem, pss, psr, rss, rsr, ags, agr, dds, ddr):
    layers = hq.shape[0]
    rows = SIDE * SIDE * act.shape[3]
    brow = act.shape[3]
    width = act.shape[4]
    head = hq.shape[3]
    tile = width // TILES
    halves = 2 * layers
    slots = CORES * halves
    scale = 1.0 / math.sqrt(head)

    t = lax.axis_index("tp")
    z = lax.axis_index("dp")
    core = lax.rem(t, CORES)
    m = CORES - 1 - core
    x = lax.rem(lax.div(t, CORES), SIDE)
    y = lax.div(t, CORES * SIDE)
    partner = t + 1 - 2 * core

    def dev(yy, xx):
        return (yy * SIDE + xx) * CORES + core

    def ring(along_x):
        me = x if along_x else y
        r, o, l = (lax.rem(me + k, SIDE) for k in (1, 2, 3))
        if along_x:
            return me, r, l, o, dev(y, r), dev(y, l), dev(y, o)
        return me, r, l, o, dev(r, x), dev(l, x), dev(o, x)

    rings = {True: ring(True), False: ring(False)}

    barrier = pltpu.get_barrier_semaphore()
    peers = [partner, *rings[True][4:], *rings[False][4:]]
    for peer in peers:
        pl.semaphore_signal(barrier, inc=1, device_id=(z, peer), device_id_type=pl.DeviceIdType.MESH)

    def weight_copies(l, kind):
        i = lax.rem(l, 2)
        if kind == 0:
            cps = [pltpu.make_async_copy(
                hq.at[l, c], wq.at[i, :, pl.ds(c * head, head)], wsem.at[l, c]) for c in range(3)]
            return cps + [pltpu.make_async_copy(ho.at[l], wo.at[i], wsem.at[l, 3])]
        return [pltpu.make_async_copy(hu.at[l], wu.at[i], wsem.at[l, 4]),
                pltpu.make_async_copy(hd.at[l], wd.at[i], wsem.at[l, 5])]

    def act_copy(c, b):
        return pltpu.make_async_copy(act.at[c, b], out.at[c, b], asem.at[c, b])

    own_copy = pltpu.make_async_copy(act.at[m, y, x], xres, asem.at[CORES, 0])
    for b in range(SIDE):
        act_copy(0, b).start()
    for cp in weight_copies(0, 0):
        cp.start()
    own_copy.start()
    for b in range(SIDE):
        act_copy(1, b).start()
    for l in range(min(2, layers)):
        for kind in range(2):
            if l + kind > 0:
                for cp in weight_copies(l, kind):
                    cp.start()

    kc[...] = jnp.zeros_like(kc)
    vc[...] = jnp.zeros_like(vc)

    def first_norm(c):
        def body(b, carry):
            act_copy(c, b).wait()
            out[c, b] = norm_rows(out[c, b].astype(F32), gain1[pl.ds(0, 1), :]).astype(BF16)
            return carry

        with jax.named_scope("first_norm"):
            lax.fori_loop(0, SIDE, body, 0)

    first_norm(0)
    with jax.named_scope("own_copy"):
        own_copy.wait()

    with jax.named_scope("barrier"):
        pl.semaphore_wait(barrier, len(peers))

    def remote(src, dst, ss, rs, peer):
        return pltpu.make_async_remote_copy(
            src_ref=src, dst_ref=dst, send_sem=ss, recv_sem=rs,
            device_id=(z, peer), device_id_type=pl.DeviceIdType.MESH)

    half = width // 2

    def cols(o):
        return pl.ds(o * half, half)

    first = [rings[True], rings[False]]
    second = [rings[False], rings[True]]

    def b2_of(o, p):
        me2, r2, l2, op2 = second[o][:4]
        return (op2, r2, l2, me2)[p]

    def rs_blk(o, b1, b2, cs):
        return part.at[b2, b1, :, cs] if o == 0 else part.at[b1, b2, :, cs]

    def parts(o):
        quarter = half // 2
        return pl.ds(o * half, quarter), pl.ds(o * half + quarter, quarter)

    def rs1(o, p, k):
        _, r, l, op, rdev, ldev, opdev = first[o]
        b, to = [(op, opdev), (r, rdev), (l, ldev)][k]
        src = rs_blk(o, b, b2_of(o, p), cols(o))
        return remote(src, fb.at[o, k, p], rss.at[o, p, k], rsr.at[o, p, k], to)

    def rs2(o, k):
        _, r, l, op, rdev, ldev, opdev = second[o]
        b, to = [(op, opdev), (r, rdev), (l, ldev)][k]
        return remote(rs_blk(o, first[o][0], b, cols(o)), gb.at[o, k], rss.at[o, 4, k], rsr.at[o, 4, k], to)

    def add_to(blk, *others):
        total = blk[...].astype(F32)
        for other in others:
            total = total + other[...].astype(F32)
        return total

    def rs1_start(o):
        for p in range(SIDE):
            for k in range(3):
                rs1(o, p, k).start()

    def rs1_sum(o, p):
        for k in range(3):
            rs1(o, p, k).wait_recv()
        blk = rs_blk(o, first[o][0], b2_of(o, p), cols(o))
        blk[...] = add_to(blk, *(fb.at[o, k, p] for k in range(3))).astype(BF16)
        if p < 3:
            rs2(o, p).start()

    def rs2_sum(o):
        full = cols(o)
        for k in range(3):
            rs2(o, k).wait_recv()
        blk = rs_blk(o, first[o][0], second[o][0], full)
        xres[:, full] = add_to(xres.at[:, full], blk, *(gb.at[o, k] for k in range(3))).astype(BF16)

    def ag_blk(o, b1, b2, cs):
        return out.at[m, b2, b1, :, cs] if o == 0 else out.at[m, b1, b2, :, cs]

    def ag1(o, k):
        to = second[o][4 + (2, 0, 1)[k]]
        ref = ag_blk(o, first[o][0], second[o][0], cols(o))
        return remote(ref, ref, ags.at[o, 4, k], agr.at[o, 4, k], to)

    def ag2(o, p, k):
        to = first[o][4 + (2, 0, 1)[k]]
        ref = ag_blk(o, first[o][0], b2_of(o, p), cols(o))
        return remote(ref, ref, ags.at[o, p, k], agr.at[o, p, k], to)

    def fwd2(o, p, k):
        _, r, l, _, rdev, ldev, _ = first[o]
        b, to = [(l, rdev), (r, ldev)][k]
        ref = ag_blk(o, b, b2_of(o, p), parts(o)[k])
        return remote(ref, ref, ags.at[o, p, 3 + k], agr.at[o, p, 3 + k], to)

    def to_partner(o, b, p, cs=None):
        ref = ag_blk(o, b, b2_of(o, p), cols(o) if cs is None else cs)
        remote(ref, ref, dds.at[0], ddr.at[0], partner).start()

    def whole(c):
        return remote(out.at[c], out.at[c], dds.at[0], ddr.at[0], partner)

    def wait_other():
        whole(1 - m).wait_recv()

    def gather_piece(o, p):
        for k in (1, 2):
            ag2(o, p, k).start()
        if p == 0:
            ag2(o, p, 0).start()
        else:
            @pl.when(m == 1)
            def _():
                ag2(o, p, 0).start()
        to_partner(o, first[o][0], p)

    def p_desc(n):
        return remote(psnd.at[n], prcv.at[n], pss.at[n], psr.at[n], partner)

    def attention(c, l):
        a = out[c].reshape(rows, width)
        qkv = jnp.dot(a, wq[lax.rem(l, 2)], preferred_element_type=F32).astype(BF16)
        base = pl.multiple_of(c * rows, rows)
        kc[pl.ds(base, rows), :] = qkv[:, head:2 * head]
        vc[pl.ds(base, rows), :] = qkv[:, 2 * head:]
        s = lax.dot_general(qkv[:, :head], kc[...], (((1,), (1,)), ((), ())),
                            preferred_element_type=F32) * scale
        q_pos = base + lax.broadcasted_iota(jnp.int32, s.shape, 0)
        k_pos = lax.broadcasted_iota(jnp.int32, s.shape, 1)
        s = jnp.where(k_pos <= q_pos, s, -1e30)
        p = jnp.exp(s - jnp.max(s, axis=-1, keepdims=True))
        mix = jnp.dot(p.astype(BF16), vc[...], preferred_element_type=F32)
        ob[...] = (mix / jnp.sum(p, axis=-1, keepdims=True)).astype(BF16)

    def mlp_up(c, l):
        def body(n, carry):
            cs = pl.ds(pl.multiple_of(n * 256, 256), 256)
            a = out[c].reshape(rows, width)
            up = jnp.dot(a, wu[lax.rem(l, 2), :, cs], preferred_element_type=F32)
            hid[:, cs] = jax.nn.gelu(up, approximate=True).astype(BF16)
            return carry
        lax.fori_loop(0, hid.shape[1] // 256, body, 0)

    def emit_tile(n, acc, own):
        @pl.when(own)
        def _():
            p_desc(n).wait_recv()
            total = (acc + prcv[n].astype(F32)).astype(BF16)
            cs = pl.ds(pl.multiple_of(n * tile, tile), tile)
            part[:, :, :, cs] = total.reshape(SIDE, SIDE, brow, tile)

        @pl.when(jnp.logical_not(own))
        def _():
            psnd[n] = acc.astype(BF16)
            p_desc(n).start()

    def down(o, l, odd, own):
        lo = o * (TILES // 2)

        def body(n, carry, lhs, w):
            cs = pl.ds(pl.multiple_of(n * tile, tile), tile)
            emit_tile(n, jnp.dot(lhs[...], w[lax.rem(l, 2), :, cs], preferred_element_type=F32), own)
            return carry

        @pl.when(odd == 0)
        def _():
            lax.fori_loop(lo, lo + TILES // 2, functools.partial(body, lhs=ob, w=wo), 0)

        @pl.when(odd == 1)
        def _():
            lax.fori_loop(lo, lo + TILES // 2, functools.partial(body, lhs=hid, w=wd), 0)

    def phase1_sums(p):
        with jax.named_scope(f"rs1_sum{p}"):
            for o in range(2):
                rs1_sum(o, p)

    def reduce_and_norm(done):
        with jax.named_scope("rs2_sum"):
            for o in range(2):
                rs2_sum(o)
        with jax.named_scope("owned_norm"):
            xs = xres[...].astype(F32)
            nxt = lax.div(lax.min(done + 1, halves - 1), 2)
            gain = jnp.where(lax.rem(done, 2) == 0, gain2[pl.ds(nxt, 1), :], gain1[pl.ds(nxt, 1), :])
            nrm = norm_rows(xs, gain)
            out[m, y, x] = jnp.where(done == halves - 1, xs, nrm).astype(BF16)

    def gather_send():
        with jax.named_scope("ag1"):
            for k in (1, 2, 0):
                for o in range(2):
                    ag1(o, k).start()
            for o in range(2):
                gather_piece(o, 3)
    def gather_pieces():
        for k in (1, 2, 0):
            with jax.named_scope(f"ag1_{k}"):
                for o in range(2):
                    ag1(o, k).wait_recv()
                    gather_piece(o, (0, 2, 1)[k])

    def gather_end(p, ks=(1, 2, 0)):
        with jax.named_scope(f"ag2_{p}"):
            for o in range(2):
                for k in ks:
                    ag2(o, p, k).wait_recv()
                    to_partner(o, first[o][(3, 2, 1)[k]], p)

    def gather_forward(p):
        with jax.named_scope(f"ag2_{p}"):
            for o in range(2):
                for k in range(2):
                    ag2(o, p, 1 + k).wait_recv()
                    fwd2(o, p, k).start()
                    to_partner(o, first[o][2 - k], p)

    def gather_forwarded(p):
        with jax.named_scope(f"ag2_{p}_forwarded"):
            for o in range(2):
                for k in range(2):
                    fwd2(o, p, k).wait_recv()
                    to_partner(o, first[o][3], p, parts(o)[k])

    def drain():
        with jax.named_scope("drain"):
            for o in range(2):
                for p in range(SIDE):
                    for k in range(3):
                        rs1(o, p, k).wait_send()
                    if p > 0:
                        @pl.when(m == 0)
                        def _():
                            for k in range(2):
                                fwd2(o, p, k).wait_send()

                        @pl.when(m == 1)
                        def _():
                            ag2(o, p, 0).wait_send()

                    for k in range(3) if p == 0 else (1, 2):
                        ag2(o, p, k).wait_send()
                for k in range(3):
                    rs2(o, k).wait_send()
                    ag1(o, k).wait_send()
            whole(m).wait_send()

    def wait_shares():
        for n in range(TILES):
            p_desc(n).wait_send()

    def slot(s, carry):
        c = lax.rem(s, CORES)
        h = lax.div(s, CORES)
        l = lax.div(h, 2)
        odd = lax.rem(h, 2)
        own = c == m
        other = c != m
        inside = s < slots
        late = jnp.logical_and(jnp.logical_and(c == 0, other), s >= 1)

        @pl.when(s == 1)
        def _():
            first_norm(1)

        coming = lax.div(s, 2 * CORES) + 1

        @pl.when(jnp.logical_and(lax.rem(s, 2 * CORES) == 0, jnp.logical_and(coming >= 2, coming < layers)))
        def _():
            for kind in range(2):
                for cp in weight_copies(coming, kind):
                    cp.start()

        @pl.when(jnp.logical_and(jnp.logical_and(inside, other), s >= CORES))
        def _():
            with jax.named_scope("wait_other"):
                wait_other()

        for kind in range(2):
            @pl.when(jnp.logical_and(inside, odd == kind))
            def _():
                @pl.when(c == 0)
                def _():
                    with jax.named_scope("weights"):
                        for cp in weight_copies(l, kind):
                            cp.wait()

                with jax.named_scope("up"):
                    (attention, mlp_up)[kind](c, l)

        @pl.when(late)
        def _():
            gather_end(3)

        @pl.when(jnp.logical_and(jnp.logical_and(inside, own), s >= CORES))
        def _():
            drain()

        @pl.when(jnp.logical_and(jnp.logical_and(inside, other), s >= CORES))
        def _():
            wait_shares()

        for o in range(2):
            @pl.when(inside)
            def _():
                with jax.named_scope("down"):
                    down(o, l, odd, own)

            @pl.when(jnp.logical_and(inside, own))
            def _():
                rs1_start(o)

            @pl.when(late)
            def _():
                for p in ((2,), (1, 0))[o]:
                    gather_end(p)

            if o == 0:
                @pl.when(jnp.logical_and(c == 1, other))
                def _():
                    phase1_sums(0)

        @pl.when(jnp.logical_and(c == 1, own))
        def _():
            phase1_sums(0)

        @pl.when(c == 1)
        def _():
            for p in range(1, SIDE):
                phase1_sums(p)
            reduce_and_norm(h)
            gather_send()
            gather_pieces()

        @pl.when(jnp.logical_and(c == 1, other))
        def _():
            gather_forward(3)
            gather_forward(2)
            gather_forward(1)
            gather_forwarded(3)
            gather_end(0)
            gather_forwarded(2)
            gather_forwarded(1)

        return carry

    lax.fori_loop(0, slots + 1, slot, 0)
    drain()
    wait_shares()

    wait_other()


def solution(mesh):
    tp = mesh.shape["tp"]

    def device_fn(act_in, w_qkv, w_out, w_up, w_down, gain_one, gain_two):
        layers, width, _, _, head = w_qkv.shape
        seq = act_in.shape[0]
        ffn = w_up.shape[2]
        rows = seq // CORES
        brow = rows // (SIDE * SIDE)
        assert tp == SIDE * SIDE * CORES
        blocks = (CORES, SIDE, SIDE, brow, width)
        q_view = jnp.transpose(w_qkv, (0, 2, 3, 1, 4)).reshape(layers, 3, width, head)
        half = width // 2
        tile = width // TILES
        vmem = pltpu.VMEM
        dma = pltpu.SemaphoreType.DMA
        hbm_spec = pl.BlockSpec(memory_space=pltpu.HBM)
        vmem_spec = pl.BlockSpec(memory_space=pltpu.VMEM)
        res = pl.pallas_call(
            stack_kernel,
            out_shape=jax.ShapeDtypeStruct(blocks, BF16),
            in_specs=[hbm_spec] * 5 + [vmem_spec] * 2,
            out_specs=vmem_spec,
            scratch_shapes=[
                vmem((2, width, 3 * head), BF16),
                vmem((2, head, width), BF16),
                vmem((2, width, ffn), BF16),
                vmem((2, ffn, width), BF16),
                vmem((SIDE, SIDE, brow, width), BF16),
                vmem((TILES, rows, tile), BF16),
                vmem((TILES, rows, tile), BF16),
                vmem((2, 3, SIDE, brow, half), BF16),
                vmem((2, 3, brow, half), BF16),
                vmem((seq, head), BF16), vmem((seq, head), BF16),
                vmem((rows, head), BF16), vmem((rows, ffn), BF16),
                vmem((brow, width), BF16),
                dma((CORES + 1, SIDE)), dma((layers, 6)),
                dma((TILES,)), dma((TILES,)),
                dma((2, SIDE + 1, 3)), dma((2, SIDE + 1, 3)),
                dma((2, SIDE + 1, 5)), dma((2, SIDE + 1, 5)),
                dma((1,)), dma((1,)),
            ],
            compiler_params=pltpu.CompilerParams(
                collective_id=0, has_side_effects=True, vmem_limit_bytes=46 * 2 ** 20),
            name="layer_stack",
        )(act_in.reshape(blocks), q_view, w_out.reshape(layers, head, width), w_up, w_down, gain_one, gain_two)
        return res.reshape(seq, width)

    return jax.shard_map(
        device_fn,
        mesh=mesh,
        in_specs=(
            P("dp", None),
            P(None, None, "tp", None, None),
            P(None, "tp", None, None),
            P(None, None, "tp"),
            P(None, "tp", None),
            P(None, None),
            P(None, None),
        ),
        out_specs=P("dp", None),
        check_vma=False,
    )
```

```python
import functools
import math
import jax
import jax.numpy as jnp
from jax import lax
from jax.experimental import pallas as pl
from jax.experimental.pallas import tpu as pltpu
from jax.sharding import PartitionSpec as P

F32 = jnp.float32
BF16 = jnp.bfloat16
SIDE = 4
CORES = 2
EARLY = (0, 1)
TILES = 8


def norm_rows(rows, gain):
    centred = rows - jnp.mean(rows, axis=-1, keepdims=True)
    var = jnp.mean(centred * centred, axis=-1, keepdims=True)
    return centred * lax.rsqrt(var + 1e-5) * gain


def stack_kernel(act, hq, ho, hu, hd, gain1, gain2, out,
                 wq, wo, wu, wd, part, psnd, prcv, fb, gb,
                 kc, vc, ob, hid, xres,
                 asem, wsem, pss, psr, rss, rsr, ags, agr, dds, ddr):
    layers = hq.shape[0]
    rows = SIDE * SIDE * act.shape[3]
    brow = act.shape[3]
    width = act.shape[4]
    head = hq.shape[3]
    tile = width // TILES
    halves = 2 * layers
    slots = CORES * halves
    scale = 1.0 / math.sqrt(head)

    t = lax.axis_index("tp")
    z = lax.axis_index("dp")
    core = lax.rem(t, CORES)
    m = CORES - 1 - core
    x = lax.rem(lax.div(t, CORES), SIDE)
    y = lax.div(t, CORES * SIDE)
    partner = t + 1 - 2 * core

    def dev(yy, xx):
        return (yy * SIDE + xx) * CORES + core

    def ring(along_x):
        me = x if along_x else y
        r, o, l = (lax.rem(me + k, SIDE) for k in (1, 2, 3))
        if along_x:
            return me, r, l, o, dev(y, r), dev(y, l), dev(y, o)
        return me, r, l, o, dev(r, x), dev(l, x), dev(o, x)

    rings = {True: ring(True), False: ring(False)}

    barrier = pltpu.get_barrier_semaphore()
    peers = [partner, *rings[True][4:], *rings[False][4:]]
    for peer in peers:
        pl.semaphore_signal(barrier, inc=1, device_id=(z, peer), device_id_type=pl.DeviceIdType.MESH)

    def weight_copies(l, kind):
        i = lax.rem(l, 2)
        if kind == 0:
            cps = [pltpu.make_async_copy(
                hq.at[l, c], wq.at[i, :, pl.ds(c * head, head)], wsem.at[l, c]) for c in range(3)]
            return cps + [pltpu.make_async_copy(ho.at[l], wo.at[i], wsem.at[l, 3])]
        return [pltpu.make_async_copy(hu.at[l], wu.at[i], wsem.at[l, 4]),
                pltpu.make_async_copy(hd.at[l], wd.at[i], wsem.at[l, 5])]

    def act_copy(c, b):
        return pltpu.make_async_copy(act.at[c, b], out.at[c, b], asem.at[c, b])

    own_copy = pltpu.make_async_copy(act.at[m, y, x], xres, asem.at[CORES, 0])
    for b in range(SIDE):
        act_copy(0, b).start()
    for cp in weight_copies(0, 0):
        cp.start()
    own_copy.start()
    for b in range(SIDE):
        act_copy(1, b).start()
    for l in range(min(2, layers)):
        for kind in range(2):
            if l + kind > 0:
                for cp in weight_copies(l, kind):
                    cp.start()

    kc[...] = jnp.zeros_like(kc)
    vc[...] = jnp.zeros_like(vc)

    def first_norm(c):
        def body(b, carry):
            act_copy(c, b).wait()
            out[c, b] = norm_rows(out[c, b].astype(F32), gain1[pl.ds(0, 1), :]).astype(BF16)
            return carry

        with jax.named_scope("first_norm"):
            lax.fori_loop(0, SIDE, body, 0)

    first_norm(0)

    with jax.named_scope("barrier"):
        pl.semaphore_wait(barrier, len(peers))

    def remote(src, dst, ss, rs, peer):
        return pltpu.make_async_remote_copy(
            src_ref=src, dst_ref=dst, send_sem=ss, recv_sem=rs,
            device_id=(z, peer), device_id_type=pl.DeviceIdType.MESH)

    half = width // 2

    def cols(o):
        return pl.ds(o * half, half)

    first = [rings[True], rings[False]]
    second = [rings[False], rings[True]]

    def b2_of(o, p):
        me2, r2, l2, op2 = second[o][:4]
        return (op2, r2, l2, me2)[p]

    def rs_blk(o, b1, b2, cs):
        return part.at[b2, b1, :, cs] if o == 0 else part.at[b1, b2, :, cs]

    def rs1(o, p, k, i=None):
        _, r, l, op, rdev, ldev, opdev = first[o]
        b, to = [(op, opdev), (r, rdev), (l, ldev)][k]
        if i is None:
            src, dst, j = rs_blk(o, b, b2_of(o, p), cols(o)), fb.at[o, k, p], k
        else:
            src, dst, j = rs_blk(o, b, b2_of(o, p), parts(o)[i]), fb.at[o, k, p, :, parts(0)[i]], 3 * i + k
        return remote(src, dst, rss.at[o, p, j], rsr.at[o, p, j], to)

    def rs1_all(o, p):
        halves_of = (0, 1) if p in EARLY else (None,)
        return [rs1(o, p, k, i) for i in halves_of for k in range(3)]

    def parts(o):
        quarter = half // 2
        return pl.ds(o * half, quarter), pl.ds(o * half + quarter, quarter)

    def rs2(o, k):
        _, r, l, op, rdev, ldev, opdev = second[o]
        b, to = [(op, opdev), (r, rdev), (l, ldev)][k]
        return remote(rs_blk(o, first[o][0], b, cols(o)), gb.at[o, k], rss.at[o, 4, k], rsr.at[o, 4, k], to)

    def add_to(blk, *others):
        total = blk[...].astype(F32)
        for other in others:
            total = total + other[...].astype(F32)
        return total

    def rs1_start(o, i):
        for p in EARLY:
            for k in range(3):
                rs1(o, p, k, i).start()
        if i == 1:
            for p in range(SIDE):
                if p not in EARLY:
                    for cp in rs1_all(o, p):
                        cp.start()

    def rs1_sum(o, p):
        for cp in rs1_all(o, p):
            cp.wait_recv()
        blk = rs_blk(o, first[o][0], b2_of(o, p), cols(o))
        blk[...] = add_to(blk, *(fb.at[o, k, p] for k in range(3))).astype(BF16)
        if p < 3:
            rs2(o, p).start()

    def rs2_sum(o):
        full = cols(o)
        for k in range(3):
            rs2(o, k).wait_recv()
        blk = rs_blk(o, first[o][0], second[o][0], full)
        xres[:, full] = add_to(xres.at[:, full], blk, *(gb.at[o, k] for k in range(3))).astype(BF16)

    def ag_blk(o, b1, b2, cs):
        return out.at[m, b2, b1, :, cs] if o == 0 else out.at[m, b1, b2, :, cs]

    def ag1(o, k):
        to = second[o][4 + (2, 0, 1)[k]]
        ref = ag_blk(o, first[o][0], second[o][0], cols(o))
        return remote(ref, ref, ags.at[o, 4, k], agr.at[o, 4, k], to)

    def ag2(o, p, k):
        to = first[o][4 + (2, 0, 1)[k]]
        ref = ag_blk(o, first[o][0], b2_of(o, p), cols(o))
        return remote(ref, ref, ags.at[o, p, k], agr.at[o, p, k], to)

    def fwd2(o, p, k):
        _, r, l, _, rdev, ldev, _ = first[o]
        b, to = [(l, rdev), (r, ldev)][k]
        ref = ag_blk(o, b, b2_of(o, p), parts(o)[k])
        return remote(ref, ref, ags.at[o, p, 3 + k], agr.at[o, p, 3 + k], to)

    def to_partner(o, b, p, cs=None):
        ref = ag_blk(o, b, b2_of(o, p), cols(o) if cs is None else cs)
        remote(ref, ref, dds.at[0], ddr.at[0], partner).start()

    def whole(c):
        return remote(out.at[c], out.at[c], dds.at[0], ddr.at[0], partner)

    def wait_other():
        whole(1 - m).wait_recv()

    def gather_piece(o, p):
        for k in (1, 2):
            ag2(o, p, k).start()
        if p == 0:
            ag2(o, p, 0).start()
        else:
            @pl.when(m == 1)
            def _():
                ag2(o, p, 0).start()
        to_partner(o, first[o][0], p)

    def p_desc(n):
        return remote(psnd.at[n], prcv.at[n], pss.at[n], psr.at[n], partner)

    def attention(c, l):
        a = out[c].reshape(rows, width)
        qkv = jnp.dot(a, wq[lax.rem(l, 2)], preferred_element_type=F32).astype(BF16)
        base = pl.multiple_of(c * rows, rows)
        kc[pl.ds(base, rows), :] = qkv[:, head:2 * head]
        vc[pl.ds(base, rows), :] = qkv[:, 2 * head:]
        s = lax.dot_general(qkv[:, :head], kc[...], (((1,), (1,)), ((), ())),
                            preferred_element_type=F32) * scale
        q_pos = base + lax.broadcasted_iota(jnp.int32, s.shape, 0)
        k_pos = lax.broadcasted_iota(jnp.int32, s.shape, 1)
        s = jnp.where(k_pos <= q_pos, s, -1e30)
        p = jnp.exp(s - jnp.max(s, axis=-1, keepdims=True))
        mix = jnp.dot(p.astype(BF16), vc[...], preferred_element_type=F32)
        ob[...] = (mix / jnp.sum(p, axis=-1, keepdims=True)).astype(BF16)

    def mlp_up(c, l):
        def body(n, carry):
            cs = pl.ds(pl.multiple_of(n * 256, 256), 256)
            a = out[c].reshape(rows, width)
            up = jnp.dot(a, wu[lax.rem(l, 2), :, cs], preferred_element_type=F32)
            hid[:, cs] = jax.nn.gelu(up, approximate=True).astype(BF16)
            return carry
        lax.fori_loop(0, hid.shape[1] // 256, body, 0)

    def emit_tile(n, acc, own):
        @pl.when(own)
        def _():
            p_desc(n).wait_recv()
            total = (acc + prcv[n].astype(F32)).astype(BF16)
            cs = pl.ds(pl.multiple_of(n * tile, tile), tile)
            part[:, :, :, cs] = total.reshape(SIDE, SIDE, brow, tile)

        @pl.when(jnp.logical_not(own))
        def _():
            psnd[n] = acc.astype(BF16)
            p_desc(n).start()

    def down(o, i, l, odd, own):
        lo = (2 * o + i) * (TILES // 4)

        def body(n, carry, lhs, w):
            cs = pl.ds(pl.multiple_of(n * tile, tile), tile)
            emit_tile(n, jnp.dot(lhs[...], w[lax.rem(l, 2), :, cs], preferred_element_type=F32), own)
            return carry

        @pl.when(odd == 0)
        def _():
            lax.fori_loop(lo, lo + TILES // 4, functools.partial(body, lhs=ob, w=wo), 0)

        @pl.when(odd == 1)
        def _():
            lax.fori_loop(lo, lo + TILES // 4, functools.partial(body, lhs=hid, w=wd), 0)

    def phase1_sums(p):
        with jax.named_scope(f"rs1_sum{p}"):
            for o in range(2):
                rs1_sum(o, p)

    def reduce_and_norm(done):
        with jax.named_scope("rs2_sum"):
            for o in range(2):
                rs2_sum(o)
        with jax.named_scope("owned_norm"):
            xs = xres[...].astype(F32)
            nxt = lax.div(lax.min(done + 1, halves - 1), 2)
            gain = jnp.where(lax.rem(done, 2) == 0, gain2[pl.ds(nxt, 1), :], gain1[pl.ds(nxt, 1), :])
            nrm = norm_rows(xs, gain)
            out[m, y, x] = jnp.where(done == halves - 1, xs, nrm).astype(BF16)

    def gather_send():
        with jax.named_scope("ag1"):
            for k in (1, 2, 0):
                for o in range(2):
                    ag1(o, k).start()
            for o in range(2):
                gather_piece(o, 3)
    def gather_pieces():
        for k in (1, 2, 0):
            with jax.named_scope(f"ag1_{k}"):
                for o in range(2):
                    ag1(o, k).wait_recv()
                    gather_piece(o, (0, 2, 1)[k])

    def gather_end(p, ks=(1, 2, 0)):
        with jax.named_scope(f"ag2_{p}"):
            for o in range(2):
                for k in ks:
                    ag2(o, p, k).wait_recv()
                    to_partner(o, first[o][(3, 2, 1)[k]], p)

    def gather_forward(p):
        with jax.named_scope(f"ag2_{p}"):
            for o in range(2):
                for k in range(2):
                    ag2(o, p, 1 + k).wait_recv()
                    fwd2(o, p, k).start()
                    to_partner(o, first[o][2 - k], p)

    def gather_forwarded(p):
        with jax.named_scope(f"ag2_{p}_forwarded"):
            for o in range(2):
                for k in range(2):
                    fwd2(o, p, k).wait_recv()
                    to_partner(o, first[o][3], p, parts(o)[k])

    def drain():
        with jax.named_scope("drain"):
            for o in range(2):
                for p in range(SIDE):
                    for cp in rs1_all(o, p):
                        cp.wait_send()
                    if p > 0:
                        @pl.when(m == 0)
                        def _():
                            for k in range(2):
                                fwd2(o, p, k).wait_send()

                        @pl.when(m == 1)
                        def _():
                            ag2(o, p, 0).wait_send()

                    for k in range(3) if p == 0 else (1, 2):
                        ag2(o, p, k).wait_send()
                for k in range(3):
                    rs2(o, k).wait_send()
                    ag1(o, k).wait_send()
            whole(m).wait_send()

    def wait_shares():
        for n in range(TILES):
            p_desc(n).wait_send()

    def slot(s, carry):
        c = lax.rem(s, CORES)
        h = lax.div(s, CORES)
        l = lax.div(h, 2)
        odd = lax.rem(h, 2)
        own = c == m
        other = c != m
        inside = s < slots
        late = jnp.logical_and(jnp.logical_and(c == 0, other), s >= 1)

        @pl.when(s == 1)
        def _():
            first_norm(1)
            own_copy.wait()

        coming = lax.div(s, 2 * CORES) + 1

        @pl.when(jnp.logical_and(lax.rem(s, 2 * CORES) == 0, jnp.logical_and(coming >= 2, coming < layers)))
        def _():
            for kind in range(2):
                for cp in weight_copies(coming, kind):
                    cp.start()

        @pl.when(jnp.logical_and(jnp.logical_and(inside, other), s >= CORES))
        def _():
            with jax.named_scope("wait_other"):
                wait_other()

        for kind in range(2):
            @pl.when(jnp.logical_and(inside, odd == kind))
            def _():
                @pl.when(c == 0)
                def _():
                    with jax.named_scope("weights"):
                        for cp in weight_copies(l, kind):
                            cp.wait()

                with jax.named_scope("up"):
                    (attention, mlp_up)[kind](c, l)

        @pl.when(late)
        def _():
            gather_end(3)

        @pl.when(jnp.logical_and(jnp.logical_and(inside, own), s >= CORES))
        def _():
            drain()

        @pl.when(jnp.logical_and(jnp.logical_and(inside, other), s >= CORES))
        def _():
            wait_shares()

        for q in range(4):
            o, i = q % 2, q // 2

            @pl.when(inside)
            def _():
                with jax.named_scope("down"):
                    down(o, i, l, odd, own)

            @pl.when(jnp.logical_and(inside, own))
            def _():
                rs1_start(o, i)

            if q in (1, 3):
                @pl.when(late)
                def _():
                    for p in {1: (2,), 3: (1, 0)}[q]:
                        gather_end(p)

            if q == 1:
                @pl.when(jnp.logical_and(c == 1, other))
                def _():
                    phase1_sums(0)

        @pl.when(jnp.logical_and(c == 1, own))
        def _():
            phase1_sums(0)

        @pl.when(c == 1)
        def _():
            for p in range(1, SIDE):
                phase1_sums(p)
            reduce_and_norm(h)
            gather_send()
            gather_pieces()

        @pl.when(jnp.logical_and(c == 1, other))
        def _():
            gather_forward(3)
            gather_forward(2)
            gather_forward(1)
            gather_forwarded(3)
            gather_end(0)
            gather_forwarded(2)
            gather_forwarded(1)

        return carry

    lax.fori_loop(0, slots + 1, slot, 0)
    drain()
    wait_shares()

    wait_other()


def solution(mesh):
    tp = mesh.shape["tp"]

    def device_fn(act_in, w_qkv, w_out, w_up, w_down, gain_one, gain_two):
        layers, width, _, _, head = w_qkv.shape
        seq = act_in.shape[0]
        ffn = w_up.shape[2]
        rows = seq // CORES
        brow = rows // (SIDE * SIDE)
        assert tp == SIDE * SIDE * CORES
        blocks = (CORES, SIDE, SIDE, brow, width)
        q_view = jnp.transpose(w_qkv, (0, 2, 3, 1, 4)).reshape(layers, 3, width, head)
        half = width // 2
        tile = width // TILES
        vmem = pltpu.VMEM
        dma = pltpu.SemaphoreType.DMA
        hbm_spec = pl.BlockSpec(memory_space=pltpu.HBM)
        vmem_spec = pl.BlockSpec(memory_space=pltpu.VMEM)
        res = pl.pallas_call(
            stack_kernel,
            out_shape=jax.ShapeDtypeStruct(blocks, BF16),
            in_specs=[hbm_spec] * 5 + [vmem_spec] * 2,
            out_specs=vmem_spec,
            scratch_shapes=[
                vmem((2, width, 3 * head), BF16),
                vmem((2, head, width), BF16),
                vmem((2, width, ffn), BF16),
                vmem((2, ffn, width), BF16),
                vmem((SIDE, SIDE, brow, width), BF16),
                vmem((TILES, rows, tile), BF16),
                vmem((TILES, rows, tile), BF16),
                vmem((2, 3, SIDE, brow, half), BF16),
                vmem((2, 3, brow, half), BF16),
                vmem((seq, head), BF16), vmem((seq, head), BF16),
                vmem((rows, head), BF16), vmem((rows, ffn), BF16),
                vmem((brow, width), BF16),
                dma((CORES + 1, SIDE)), dma((layers, 6)),
                dma((TILES,)), dma((TILES,)),
                dma((2, SIDE + 1, 6)), dma((2, SIDE + 1, 6)),
                dma((2, SIDE + 1, 5)), dma((2, SIDE + 1, 5)),
                dma((1,)), dma((1,)),
            ],
            compiler_params=pltpu.CompilerParams(
                collective_id=0, has_side_effects=True, vmem_limit_bytes=46 * 2 ** 20),
            name="layer_stack",
        )(act_in.reshape(blocks), q_view, w_out.reshape(layers, head, width), w_up, w_down, gain_one, gain_two)
        return res.reshape(seq, width)

    return jax.shard_map(
        device_fn,
        mesh=mesh,
        in_specs=(
            P("dp", None),
            P(None, None, "tp", None, None),
            P(None, "tp", None, None),
            P(None, None, "tp"),
            P(None, "tp", None),
            P(None, None),
            P(None, None),
        ),
        out_specs=P("dp", None),
        check_vma=False,
    )
```

```python
import functools
import math
import jax
import jax.numpy as jnp
from jax import lax
from jax.experimental import pallas as pl
from jax.experimental.pallas import tpu as pltpu
from jax.sharding import PartitionSpec as P

F32 = jnp.float32
BF16 = jnp.bfloat16
SIDE = 4
CORES = 2
EARLY = (0, 1)
TILES = 8


def norm_rows(rows, gain):
    centred = rows - jnp.mean(rows, axis=-1, keepdims=True)
    var = jnp.mean(centred * centred, axis=-1, keepdims=True)
    return centred * lax.rsqrt(var + 1e-5) * gain


def stack_kernel(act, hq, ho, hu, hd, hg1, hg2, out,
                 wq, wo, wu, wd, part, psnd, prcv, fb, gb,
                 kc, vc, ob, hid, xres, gain1, gain2,
                 asem, wsem, pss, psr, rss, rsr, ags, agr, dds, ddr):
    layers = hq.shape[0]
    rows = SIDE * SIDE * act.shape[3]
    brow = act.shape[3]
    width = act.shape[4]
    head = hq.shape[3]
    tile = width // TILES
    halves = 2 * layers
    slots = CORES * halves
    scale = 1.0 / math.sqrt(head)

    t = lax.axis_index("tp")
    z = lax.axis_index("dp")
    core = lax.rem(t, CORES)
    m = CORES - 1 - core
    x = lax.rem(lax.div(t, CORES), SIDE)
    y = lax.div(t, CORES * SIDE)
    partner = t + 1 - 2 * core

    def dev(yy, xx):
        return (yy * SIDE + xx) * CORES + core

    def ring(along_x):
        me = x if along_x else y
        r, o, l = (lax.rem(me + k, SIDE) for k in (1, 2, 3))
        if along_x:
            return me, r, l, o, dev(y, r), dev(y, l), dev(y, o)
        return me, r, l, o, dev(r, x), dev(l, x), dev(o, x)

    rings = {True: ring(True), False: ring(False)}

    barrier = pltpu.get_barrier_semaphore()
    peers = [partner, *rings[True][4:], *rings[False][4:]]
    for peer in peers:
        pl.semaphore_signal(barrier, inc=1, device_id=(z, peer), device_id_type=pl.DeviceIdType.MESH)

    def weight_copies(l, kind):
        i = lax.rem(l, 2)
        if kind == 0:
            cps = [pltpu.make_async_copy(
                hq.at[l, c], wq.at[i, :, pl.ds(c * head, head)], wsem.at[l, c]) for c in range(3)]
            return cps + [pltpu.make_async_copy(ho.at[l], wo.at[i], wsem.at[l, 3])]
        return [pltpu.make_async_copy(hu.at[l], wu.at[i], wsem.at[l, 4]),
                pltpu.make_async_copy(hd.at[l], wd.at[i], wsem.at[l, 5])]

    def act_copy(c, b):
        return pltpu.make_async_copy(act.at[c, b], out.at[c, b], asem.at[c, b])

    gain_copies = [pltpu.make_async_copy(hg1, gain1, asem.at[CORES, 1]),
                   pltpu.make_async_copy(hg2, gain2, asem.at[CORES, 2])]
    own_copy = pltpu.make_async_copy(act.at[m, y, x], xres, asem.at[CORES, 0])
    for cp in gain_copies:
        cp.start()
    for b in range(SIDE):
        act_copy(0, b).start()
    for cp in weight_copies(0, 0):
        cp.start()
    own_copy.start()
    for b in range(SIDE):
        act_copy(1, b).start()
    for l in range(min(2, layers)):
        for kind in range(2):
            if l + kind > 0:
                for cp in weight_copies(l, kind):
                    cp.start()

    kc[...] = jnp.zeros_like(kc)
    vc[...] = jnp.zeros_like(vc)

    def first_norm(c):
        def body(b, carry):
            act_copy(c, b).wait()
            out[c, b] = norm_rows(out[c, b].astype(F32), gain1[pl.ds(0, 1), :]).astype(BF16)
            return carry

        with jax.named_scope("first_norm"):
            lax.fori_loop(0, SIDE, body, 0)

    for cp in gain_copies:
        cp.wait()
    first_norm(0)

    with jax.named_scope("barrier"):
        pl.semaphore_wait(barrier, len(peers))

    def remote(src, dst, ss, rs, peer):
        return pltpu.make_async_remote_copy(
            src_ref=src, dst_ref=dst, send_sem=ss, recv_sem=rs,
            device_id=(z, peer), device_id_type=pl.DeviceIdType.MESH)

    half = width // 2

    def cols(o):
        return pl.ds(o * half, half)

    first = [rings[True], rings[False]]
    second = [rings[False], rings[True]]

    def b2_of(o, p):
        me2, r2, l2, op2 = second[o][:4]
        return (op2, r2, l2, me2)[p]

    def rs_blk(o, b1, b2, cs):
        return part.at[b2, b1, :, cs] if o == 0 else part.at[b1, b2, :, cs]

    def rs1(o, p, k, i=None):
        _, r, l, op, rdev, ldev, opdev = first[o]
        b, to = [(op, opdev), (r, rdev), (l, ldev)][k]
        if i is None:
            src, dst, j = rs_blk(o, b, b2_of(o, p), cols(o)), fb.at[o, k, p], k
        else:
            src, dst, j = rs_blk(o, b, b2_of(o, p), parts(o)[i]), fb.at[o, k, p, :, parts(0)[i]], 3 * i + k
        return remote(src, dst, rss.at[o, p, j], rsr.at[o, p, j], to)

    def rs1_all(o, p):
        halves_of = (0, 1) if p in EARLY else (None,)
        return [rs1(o, p, k, i) for i in halves_of for k in range(3)]

    def parts(o):
        quarter = half // 2
        return pl.ds(o * half, quarter), pl.ds(o * half + quarter, quarter)

    def rs2(o, k):
        _, r, l, op, rdev, ldev, opdev = second[o]
        b, to = [(op, opdev), (r, rdev), (l, ldev)][k]
        return remote(rs_blk(o, first[o][0], b, cols(o)), gb.at[o, k], rss.at[o, 4, k], rsr.at[o, 4, k], to)

    def add_to(blk, *others):
        total = blk[...].astype(F32)
        for other in others:
            total = total + other[...].astype(F32)
        return total

    def rs1_start(o, i):
        for p in EARLY:
            for k in range(3):
                rs1(o, p, k, i).start()
        if i == 1:
            for p in range(SIDE):
                if p not in EARLY:
                    for cp in rs1_all(o, p):
                        cp.start()

    def rs1_sum(o, p):
        for cp in rs1_all(o, p):
            cp.wait_recv()
        blk = rs_blk(o, first[o][0], b2_of(o, p), cols(o))
        blk[...] = add_to(blk, *(fb.at[o, k, p] for k in range(3))).astype(BF16)
        if p < 3:
            rs2(o, p).start()

    def rs2_sum(o):
        full = cols(o)
        for k in range(3):
            rs2(o, k).wait_recv()
        blk = rs_blk(o, first[o][0], second[o][0], full)
        xres[:, full] = add_to(xres.at[:, full], blk, *(gb.at[o, k] for k in range(3))).astype(BF16)

    def ag_blk(o, b1, b2, cs):
        return out.at[m, b2, b1, :, cs] if o == 0 else out.at[m, b1, b2, :, cs]

    def ag1(o, k):
        to = second[o][4 + (2, 0, 1)[k]]
        ref = ag_blk(o, first[o][0], second[o][0], cols(o))
        return remote(ref, ref, ags.at[o, 4, k], agr.at[o, 4, k], to)

    def ag2(o, p, k):
        to = first[o][4 + (2, 0, 1)[k]]
        ref = ag_blk(o, first[o][0], b2_of(o, p), cols(o))
        return remote(ref, ref, ags.at[o, p, k], agr.at[o, p, k], to)

    def fwd2(o, p, k):
        _, r, l, _, rdev, ldev, _ = first[o]
        b, to = [(l, rdev), (r, ldev)][k]
        ref = ag_blk(o, b, b2_of(o, p), parts(o)[k])
        return remote(ref, ref, ags.at[o, p, 3 + k], agr.at[o, p, 3 + k], to)

    def to_partner(o, b, p, cs=None):
        ref = ag_blk(o, b, b2_of(o, p), cols(o) if cs is None else cs)
        remote(ref, ref, dds.at[0], ddr.at[0], partner).start()

    def whole(c):
        return remote(out.at[c], out.at[c], dds.at[0], ddr.at[0], partner)

    def wait_other():
        whole(1 - m).wait_recv()

    def gather_piece(o, p):
        for k in (1, 2):
            ag2(o, p, k).start()
        if p == 0:
            ag2(o, p, 0).start()
        else:
            @pl.when(m == 1)
            def _():
                ag2(o, p, 0).start()
        to_partner(o, first[o][0], p)

    def p_desc(n):
        return remote(psnd.at[n], prcv.at[n], pss.at[n], psr.at[n], partner)

    def attention(c, l):
        a = out[c].reshape(rows, width)
        qkv = jnp.dot(a, wq[lax.rem(l, 2)], preferred_element_type=F32).astype(BF16)
        base = pl.multiple_of(c * rows, rows)
        kc[pl.ds(base, rows), :] = qkv[:, head:2 * head]
        vc[pl.ds(base, rows), :] = qkv[:, 2 * head:]
        s = lax.dot_general(qkv[:, :head], kc[...], (((1,), (1,)), ((), ())),
                            preferred_element_type=F32) * scale
        q_pos = base + lax.broadcasted_iota(jnp.int32, s.shape, 0)
        k_pos = lax.broadcasted_iota(jnp.int32, s.shape, 1)
        s = jnp.where(k_pos <= q_pos, s, -1e30)
        p = jnp.exp(s - jnp.max(s, axis=-1, keepdims=True))
        mix = jnp.dot(p.astype(BF16), vc[...], preferred_element_type=F32)
        ob[...] = (mix / jnp.sum(p, axis=-1, keepdims=True)).astype(BF16)

    def mlp_up(c, l):
        def body(n, carry):
            cs = pl.ds(pl.multiple_of(n * 256, 256), 256)
            a = out[c].reshape(rows, width)
            up = jnp.dot(a, wu[lax.rem(l, 2), :, cs], preferred_element_type=F32)
            hid[:, cs] = jax.nn.gelu(up, approximate=True).astype(BF16)
            return carry
        lax.fori_loop(0, hid.shape[1] // 256, body, 0)

    def emit_tile(n, acc, own):
        @pl.when(own)
        def _():
            p_desc(n).wait_recv()
            total = (acc + prcv[n].astype(F32)).astype(BF16)
            cs = pl.ds(pl.multiple_of(n * tile, tile), tile)
            part[:, :, :, cs] = total.reshape(SIDE, SIDE, brow, tile)

        @pl.when(jnp.logical_not(own))
        def _():
            psnd[n] = acc.astype(BF16)
            p_desc(n).start()

    def down(o, i, l, odd, own):
        lo = (2 * o + i) * (TILES // 4)

        def body(n, carry, lhs, w):
            cs = pl.ds(pl.multiple_of(n * tile, tile), tile)
            emit_tile(n, jnp.dot(lhs[...], w[lax.rem(l, 2), :, cs], preferred_element_type=F32), own)
            return carry

        @pl.when(odd == 0)
        def _():
            lax.fori_loop(lo, lo + TILES // 4, functools.partial(body, lhs=ob, w=wo), 0)

        @pl.when(odd == 1)
        def _():
            lax.fori_loop(lo, lo + TILES // 4, functools.partial(body, lhs=hid, w=wd), 0)

    def phase1_sums(p):
        with jax.named_scope(f"rs1_sum{p}"):
            for o in range(2):
                rs1_sum(o, p)

    def reduce_and_norm(done):
        with jax.named_scope("rs2_sum"):
            for o in range(2):
                rs2_sum(o)
        with jax.named_scope("owned_norm"):
            xs = xres[...].astype(F32)
            nxt = lax.div(lax.min(done + 1, halves - 1), 2)
            gain = jnp.where(lax.rem(done, 2) == 0, gain2[pl.ds(nxt, 1), :], gain1[pl.ds(nxt, 1), :])
            nrm = norm_rows(xs, gain)
            out[m, y, x] = jnp.where(done == halves - 1, xs, nrm).astype(BF16)

    def gather_send():
        with jax.named_scope("ag1"):
            for k in (1, 2, 0):
                for o in range(2):
                    ag1(o, k).start()
            for o in range(2):
                gather_piece(o, 3)
    def gather_pieces():
        for k in (1, 2, 0):
            with jax.named_scope(f"ag1_{k}"):
                for o in range(2):
                    ag1(o, k).wait_recv()
                    gather_piece(o, (0, 2, 1)[k])

    def gather_end(p, ks=(1, 2, 0)):
        with jax.named_scope(f"ag2_{p}"):
            for o in range(2):
                for k in ks:
                    ag2(o, p, k).wait_recv()
                    to_partner(o, first[o][(3, 2, 1)[k]], p)

    def gather_forward(p):
        with jax.named_scope(f"ag2_{p}"):
            for o in range(2):
                for k in range(2):
                    ag2(o, p, 1 + k).wait_recv()
                    fwd2(o, p, k).start()
                    to_partner(o, first[o][2 - k], p)

    def gather_forwarded(p):
        with jax.named_scope(f"ag2_{p}_forwarded"):
            for o in range(2):
                for k in range(2):
                    fwd2(o, p, k).wait_recv()
                    to_partner(o, first[o][3], p, parts(o)[k])

    def drain():
        with jax.named_scope("drain"):
            for o in range(2):
                for p in range(SIDE):
                    for cp in rs1_all(o, p):
                        cp.wait_send()
                    if p > 0:
                        @pl.when(m == 0)
                        def _():
                            for k in range(2):
                                fwd2(o, p, k).wait_send()

                        @pl.when(m == 1)
                        def _():
                            ag2(o, p, 0).wait_send()

                    for k in range(3) if p == 0 else (1, 2):
                        ag2(o, p, k).wait_send()
                for k in range(3):
                    rs2(o, k).wait_send()
                    ag1(o, k).wait_send()
            whole(m).wait_send()

    def wait_shares():
        for n in range(TILES):
            p_desc(n).wait_send()

    def slot(s, carry):
        c = lax.rem(s, CORES)
        h = lax.div(s, CORES)
        l = lax.div(h, 2)
        odd = lax.rem(h, 2)
        own = c == m
        other = c != m
        inside = s < slots
        late = jnp.logical_and(jnp.logical_and(c == 0, other), s >= 1)

        @pl.when(s == 1)
        def _():
            first_norm(1)
            own_copy.wait()

        coming = lax.div(s, 2 * CORES) + 1

        @pl.when(jnp.logical_and(lax.rem(s, 2 * CORES) == 0, jnp.logical_and(coming >= 2, coming < layers)))
        def _():
            for kind in range(2):
                for cp in weight_copies(coming, kind):
                    cp.start()

        @pl.when(jnp.logical_and(jnp.logical_and(inside, other), s >= CORES))
        def _():
            with jax.named_scope("wait_other"):
                wait_other()

        for kind in range(2):
            @pl.when(jnp.logical_and(inside, odd == kind))
            def _():
                @pl.when(c == 0)
                def _():
                    with jax.named_scope("weights"):
                        for cp in weight_copies(l, kind):
                            cp.wait()

                with jax.named_scope("up"):
                    (attention, mlp_up)[kind](c, l)

        @pl.when(late)
        def _():
            gather_end(3)

        @pl.when(jnp.logical_and(jnp.logical_and(inside, own), s >= CORES))
        def _():
            drain()

        @pl.when(jnp.logical_and(jnp.logical_and(inside, other), s >= CORES))
        def _():
            wait_shares()

        for q in range(4):
            o, i = q % 2, q // 2

            @pl.when(inside)
            def _():
                with jax.named_scope("down"):
                    down(o, i, l, odd, own)

            @pl.when(jnp.logical_and(inside, own))
            def _():
                rs1_start(o, i)

            if q in (1, 3):
                @pl.when(late)
                def _():
                    for p in {1: (2,), 3: (1, 0)}[q]:
                        gather_end(p)

            if q in (1, 2):
                @pl.when(jnp.logical_and(c == 1, other))
                def _():
                    phase1_sums(q - 1)

        @pl.when(jnp.logical_and(c == 1, own))
        def _():
            phase1_sums(0)

        @pl.when(c == 1)
        def _():
            @pl.when(own)
            def _():
                phase1_sums(1)

            for p in range(2, SIDE):
                phase1_sums(p)
            reduce_and_norm(h)
            gather_send()
            gather_pieces()

        @pl.when(jnp.logical_and(c == 1, other))
        def _():
            gather_forward(3)
            gather_forward(2)
            gather_forward(1)
            gather_forwarded(3)
            gather_end(0)
            gather_forwarded(2)
            gather_forwarded(1)

        return carry

    lax.fori_loop(0, slots + 1, slot, 0)
    drain()
    wait_shares()

    wait_other()


def solution(mesh):
    tp = mesh.shape["tp"]

    def device_fn(act_in, w_qkv, w_out, w_up, w_down, gain_one, gain_two):
        layers, width, _, _, head = w_qkv.shape
        seq = act_in.shape[0]
        ffn = w_up.shape[2]
        rows = seq // CORES
        brow = rows // (SIDE * SIDE)
        assert tp == SIDE * SIDE * CORES
        blocks = (CORES, SIDE, SIDE, brow, width)
        q_view = jnp.transpose(w_qkv, (0, 2, 3, 1, 4)).reshape(layers, 3, width, head)
        half = width // 2
        tile = width // TILES
        vmem = pltpu.VMEM
        dma = pltpu.SemaphoreType.DMA
        hbm_spec = pl.BlockSpec(memory_space=pltpu.HBM)
        vmem_spec = pl.BlockSpec(memory_space=pltpu.VMEM)
        def pin(array):
            return pltpu.with_memory_space_constraint(array, pltpu.HBM)

        res = pl.pallas_call(
            stack_kernel,
            out_shape=jax.ShapeDtypeStruct(blocks, BF16),
            in_specs=[hbm_spec] * 7,
            out_specs=vmem_spec,
            scratch_shapes=[
                vmem((2, width, 3 * head), BF16),
                vmem((2, head, width), BF16),
                vmem((2, width, ffn), BF16),
                vmem((2, ffn, width), BF16),
                vmem((SIDE, SIDE, brow, width), BF16),
                vmem((TILES, rows, tile), BF16),
                vmem((TILES, rows, tile), BF16),
                vmem((2, 3, SIDE, brow, half), BF16),
                vmem((2, 3, brow, half), BF16),
                vmem((seq, head), BF16), vmem((seq, head), BF16),
                vmem((rows, head), BF16), vmem((rows, ffn), BF16),
                vmem((brow, width), BF16),
                vmem((layers, width), F32), vmem((layers, width), F32),
                dma((CORES + 1, SIDE)), dma((layers, 6)),
                dma((TILES,)), dma((TILES,)),
                dma((2, SIDE + 1, 6)), dma((2, SIDE + 1, 6)),
                dma((2, SIDE + 1, 5)), dma((2, SIDE + 1, 5)),
                dma((1,)), dma((1,)),
            ],
            compiler_params=pltpu.CompilerParams(
                collective_id=0, has_side_effects=True, vmem_limit_bytes=46 * 2 ** 20),
            name="layer_stack",
        )(act_in.reshape(blocks), q_view, pin(w_out.reshape(layers, head, width)), w_up, w_down,
          pin(gain_one), pin(gain_two))
        return res.reshape(seq, width)

    return jax.shard_map(
        device_fn,
        mesh=mesh,
        in_specs=(
            P("dp", None),
            P(None, None, "tp", None, None),
            P(None, "tp", None, None),
            P(None, None, "tp"),
            P(None, "tp", None),
            P(None, None),
            P(None, None),
        ),
        out_specs=P("dp", None),
        check_vma=False,
    )
```
